64 devices in a mesh: dp: 4 (over x, y), ep: 16 (over z, core).
Axes of the slice: x: 2, y: 2, z: 8, core: 2. Of those that a mesh axis runs over, the one named last changes fastest.
The devices are a block of a 4x4x8 slice.
Arguments:
- tokens: bfloat16 [64, 512, 1024], P(('dp', 'ep')), parts along dimension 0
- w_query: bfloat16 [1024, 16, 64], P('ep')
- w_key: bfloat16 [1024, 16, 64], P('ep')
- w_value: bfloat16 [1024, 16, 64], P('ep')
- w_out: bfloat16 [1024, 1024], P('ep')
- w_router: float32 [1024, 32], replicated
- w_one: bfloat16 [32, 1024, 512], P('ep')
- w_three: bfloat16 [32, 1024, 512], P('ep')
- w_two: bfloat16 [32, 512, 1024], P('ep')
- expert_ids: int32 [64, 512, 8], P(('dp', 'ep')), parts along dimension 0
Outputs:
- output: bfloat16 [64, 512, 1024], P(('dp', 'ep')), parts along dimension 0
There are 4 independent parts. The reference program is written for one: setup_inputs(seed, part) draws one part's arguments, and reference() takes and returns one part's arrays. A program takes and returns all parts, laid end to end along the dimension named above; an argument that names none is the same for every part.
All inputs are finite; a program needn't handle non-finite values.
Results may differ from the reference program's by a relative error of at most 0.00981771.
Values are sent between devices in bfloat16 or wider.
A program may use at most 768 MiB of HBM per device.

```python
import jax
import jax.numpy as jnp
import numpy as np
from jax import lax

D = 1024
HEADS = 16
HEAD = 64
EXPERTS = 32
TOP = 8
FF = 512
TOK_DEV = 512
SEQ = 512
GROUP = 16

TOKENS = TOK_DEV * GROUP
N_SEQ = TOKENS // SEQ
CAP = 2 * TOK_DEV * TOP // EXPERTS
WIDTH = HEADS * HEAD
EPS = 1e-6


def draw_routing(route_key):
    mean_load = TOK_DEV * TOP // EXPERTS
    ranks = np.arange(EXPERTS)
    loads = np.where(ranks < EXPERTS // 4, 2 * mean_load, np.where(ranks < EXPERTS // 2, mean_load, mean_load // 2))
    rank_of_pos = np.repeat(ranks, loads)
    order_key, device_key = jax.random.split(route_key)
    expert_order = jax.random.permutation(order_key, EXPERTS)
    grid = expert_order[rank_of_pos].reshape(TOP, TOK_DEV).T

    def one_device(dev_key):
        perm_key, shift_key = jax.random.split(dev_key)
        token_order = jax.random.permutation(perm_key, TOK_DEV)
        shift = jax.random.randint(shift_key, (TOK_DEV, 1), 0, TOP)
        columns = (jnp.arange(TOP)[None, :] + shift) % TOP
        return jnp.take_along_axis(grid[token_order], columns, axis=1)

    routes = jax.vmap(one_device)(jax.random.split(device_key, GROUP))
    return routes.reshape(N_SEQ, SEQ, TOP).astype(jnp.int32)


def setup_inputs(seed: int = 0, part: int = 0) -> dict:
    root_key = jax.random.key(seed)
    part_keys = jax.random.split(jax.random.fold_in(root_key, part), 3)
    weight_keys = jax.random.split(root_key, 8)

    def gaussian(index, shape, scale):
        return scale * jax.random.normal(weight_keys[index], shape, jnp.float32)

    seq_base = jax.random.normal(part_keys[0], (N_SEQ, 1, D), jnp.float32)
    noise = jax.random.normal(part_keys[1], (N_SEQ, SEQ, D), jnp.float32)
    return {
        'tokens': (0.6 * seq_base + 0.8 * noise).astype(jnp.bfloat16),
        'w_query': gaussian(0, (D, HEADS, HEAD), 1.5 * D ** -0.5).astype(jnp.bfloat16),
        'w_key': gaussian(1, (D, HEADS, HEAD), 1.5 * D ** -0.5).astype(jnp.bfloat16),
        'w_value': gaussian(2, (D, HEADS, HEAD), D ** -0.5).astype(jnp.bfloat16),
        'w_out': gaussian(3, (WIDTH, D), WIDTH ** -0.5).astype(jnp.bfloat16),
        'w_router': gaussian(4, (D, EXPERTS), D ** -0.5),
        'w_one': gaussian(5, (EXPERTS, D, FF), D ** -0.5).astype(jnp.bfloat16),
        'w_three': gaussian(6, (EXPERTS, D, FF), D ** -0.5).astype(jnp.bfloat16),
        'w_two': gaussian(7, (EXPERTS, FF, D), 2.0 * FF ** -0.5).astype(jnp.bfloat16),
        'expert_ids': draw_routing(part_keys[2]),
    }


def rms_norm(vals):
    wide = vals.astype(jnp.float32)
    return wide * lax.rsqrt(jnp.mean(wide * wide, axis=-1, keepdims=True) + EPS)


def reference(tokens, w_query, w_key, w_value, w_out, w_router, w_one, w_three, w_two, expert_ids):
    flat_query = w_query.reshape(D, WIDTH)
    flat_key = w_key.reshape(D, WIDTH)
    flat_value = w_value.reshape(D, WIDTH)
    causal = jnp.arange(SEQ)[:, None] >= jnp.arange(SEQ)[None, :]

    def one_sequence(seq_tokens):
        normed = rms_norm(seq_tokens).astype(jnp.bfloat16)
        query = jnp.dot(normed, flat_query, preferred_element_type=jnp.float32).astype(jnp.bfloat16)
        keys = jnp.dot(normed, flat_key, preferred_element_type=jnp.float32).astype(jnp.bfloat16)
        values = jnp.dot(normed, flat_value, preferred_element_type=jnp.float32).astype(jnp.bfloat16)
        query = query.astype(jnp.float32).reshape(SEQ, HEADS, HEAD)
        keys = keys.astype(jnp.float32).reshape(SEQ, HEADS, HEAD)
        values = values.astype(jnp.float32).reshape(SEQ, HEADS, HEAD)
        scores = jnp.einsum('qhk,shk->hqs', query, keys) * HEAD ** -0.5
        scores = jnp.where(causal, scores, -jnp.inf)
        attn_weights = jax.nn.softmax(scores, axis=-1).astype(jnp.bfloat16).astype(jnp.float32)
        context = jnp.einsum('hqs,shk->qhk', attn_weights, values).astype(jnp.bfloat16)
        attn_out = jnp.dot(context.reshape(SEQ, WIDTH), w_out, preferred_element_type=jnp.float32)
        return (seq_tokens.astype(jnp.float32) + attn_out).astype(jnp.bfloat16)

    hidden = lax.map(one_sequence, tokens).reshape(TOKENS, D)
    normed = rms_norm(hidden)
    logits = jnp.dot(normed, w_router, preferred_element_type=jnp.float32)
    ids_flat = expert_ids.reshape(TOKENS, TOP)
    gates = jax.nn.softmax(jnp.take_along_axis(logits, ids_flat, axis=1), axis=-1)
    padded = jnp.concatenate([normed.astype(jnp.bfloat16), jnp.zeros((1, D), jnp.bfloat16)], axis=0)
    limit = GROUP * CAP

    def one_expert(total_mix, expert_pack):
        expert, first_w, third_w, second_w = expert_pack
        match = ids_flat == expert
        weight = jnp.sum(jnp.where(match, gates, 0.0), axis=1)
        rows = jnp.nonzero(jnp.any(match, axis=1), size=limit, fill_value=TOKENS)[0]
        picked = padded[rows]
        first = jnp.dot(picked, first_w, preferred_element_type=jnp.float32)
        third = jnp.dot(picked, third_w, preferred_element_type=jnp.float32)
        activated = (jax.nn.silu(first) * third).astype(jnp.bfloat16)
        result = jnp.dot(activated, second_w, preferred_element_type=jnp.float32).astype(jnp.bfloat16)
        scale = jnp.concatenate([weight, jnp.zeros((1,), jnp.float32)])[rows]
        total_mix = total_mix.at[rows].add(scale[:, None] * result.astype(jnp.float32), mode='drop')
        return total_mix, None

    total_mix, _ = lax.scan(one_expert, jnp.zeros((TOKENS, D), jnp.float32), (jnp.arange(EXPERTS), w_one, w_three, w_two))
    layer_out = (hidden.astype(jnp.float32) + total_mix).astype(jnp.bfloat16)
    return layer_out.reshape(N_SEQ, SEQ, D)
```

```python
import functools

import jax
import jax.numpy as jnp
from jax import lax
from jax.experimental import pallas as pl
from jax.experimental.pallas import tpu as pltpu
from jax.sharding import PartitionSpec as P

EPS = 1e-6
MESH = pl.DeviceIdType.MESH


def rms_norm(vals):
    wide = vals.astype(jnp.float32)
    return wide * lax.rsqrt(jnp.mean(wide * wide, axis=-1, keepdims=True) + EPS)


def attention_layer(tokens, w_query, w_key, w_value, w_out):
    seq_count = tokens.shape[0]
    seq_len = tokens.shape[1]
    head_dim = w_query.shape[2]
    normed = rms_norm(tokens).astype(jnp.bfloat16)
    query = jnp.einsum('bsd,dhk->bshk', normed, w_query, preferred_element_type=jnp.float32).astype(jnp.bfloat16)
    keys = jnp.einsum('bsd,dhk->bshk', normed, w_key, preferred_element_type=jnp.float32).astype(jnp.bfloat16)
    values = jnp.einsum('bsd,dhk->bshk', normed, w_value, preferred_element_type=jnp.float32).astype(jnp.bfloat16)
    scores = jnp.einsum('bqhk,bshk->bhqs', query, keys, preferred_element_type=jnp.float32) * head_dim ** -0.5
    causal = lax.broadcasted_iota(jnp.int32, (seq_len, seq_len), 0) >= lax.broadcasted_iota(jnp.int32, (seq_len, seq_len), 1)
    attn_weights = jax.nn.softmax(jnp.where(causal, scores, -jnp.inf), axis=-1).astype(jnp.bfloat16)
    context = jnp.einsum('bhqs,bshk->bqhk', attn_weights, values, preferred_element_type=jnp.float32).astype(jnp.bfloat16)
    attn_out = jnp.einsum('crd,de->cre', context.reshape(seq_count, seq_len, -1), w_out, preferred_element_type=jnp.float32)
    return (tokens.astype(jnp.float32) + attn_out).astype(jnp.bfloat16)


def router_gates(hidden, w_router, expert_ids):
    normed = rms_norm(hidden)
    logits = jnp.dot(normed, w_router, precision=lax.Precision.HIGHEST, preferred_element_type=jnp.float32)
    chosen = jnp.take_along_axis(logits, expert_ids, axis=-1)
    gates = jax.nn.softmax(chosen, axis=-1)
    experts = w_router.shape[1]
    match = expert_ids[:, :, None] == jnp.arange(experts, dtype=jnp.int32)
    dense = jnp.sum(jnp.where(match, gates[:, :, None], 0.0), axis=1)
    return normed.astype(jnp.bfloat16), dense.T


def moe_kernel(n, hops, u_hbm, g_ref, h_ref, w1_hbm, w3_hbm, w2_hbm, y_ref,
               ubuf, gbuf, part, acc, w1, w3, w2,
               u_send, u_recv, a_send, a_recv, g_send, g_recv, w_send, w_recv, w_loc, u_loc, *, pieces_u, pieces_a):
    me = lax.axis_index('ep')
    pos, core = lax.div(me, 2), lax.rem(me, 2)
    tok, half = ubuf.shape[1], ubuf.shape[1] // 2
    own = w1_hbm.shape[0]
    total = w1.shape[0]
    ru, ra = half // pieces_u, half // pieces_a

    def peer(z):
        return {'ep': lax.rem(z + 2 * n, n) * 2 + core}

    sibling = {'ep': pos * 2 + (1 - core)}

    barrier = pltpu.get_barrier_semaphore()
    for k in range(1, n):
        pl.semaphore_signal(barrier, inc=1, device_id=peer(pos + k), device_id_type=MESH)
    pl.semaphore_signal(barrier, inc=1, device_id=sibling, device_id_type=MESH)

    own_copy = pltpu.make_async_copy(u_hbm, ubuf.at[0], u_loc.at[0])
    own_copy.start()
    mine = pl.ds(core * own, own)
    loads = []
    for i, (src, dst) in enumerate(((w1_hbm, w1), (w3_hbm, w3), (w2_hbm, w2))):
        loads.append(pltpu.make_async_copy(src, dst.at[mine], w_loc.at[i]))
        loads[-1].start()
    pl.semaphore_wait(barrier, n)

    def u_copy(d, s, p):
        rows = pl.ds(d * half + p * ru, ru)
        return pltpu.make_async_remote_copy(
            src_ref=ubuf.at[s, rows], dst_ref=ubuf.at[s + 1, rows],
            send_sem=u_send.at[d, s, p], recv_sem=u_recv.at[d, s, p],
            device_id=peer(pos + (1 if d == 0 else n - 1)), device_id_type=MESH)

    def a_copy(d, s, p):
        rows = pl.ds(d * half + p * ra, ra)
        return pltpu.make_async_remote_copy(
            src_ref=part.at[s, rows], dst_ref=acc.at[s - 1, rows],
            send_sem=a_send.at[d, s - 1, p], recv_sem=a_recv.at[d, s - 1, p],
            device_id=peer(pos + (n - 1 if d == 0 else 1)), device_id_type=MESH)

    def g_copy(d, s):
        cols = pl.ds(d * half, half)
        target = pos + (s if d == 0 else n - s)
        return pltpu.make_async_remote_copy(
            src_ref=g_ref.at[lax.rem(target, g_ref.shape[0]), :, cols], dst_ref=gbuf.at[s - 1, :, cols],
            send_sem=g_send.at[d, s - 1], recv_sem=g_recv.at[d, s - 1],
            device_id=peer(target), device_id_type=MESH)

    def w_copy(i, src, dst):
        return pltpu.make_async_remote_copy(
            src_ref=src, dst_ref=dst.at[mine], send_sem=w_send.at[i], recv_sem=w_recv.at[i],
            device_id=sibling, device_id_type=MESH)

    own_copy.wait()
    for p in range(pieces_u):
        for d in range(2):
            u_copy(d, 0, p).start()
    w_copies = [w_copy(i, s, t) for i, (s, t) in enumerate(((w1_hbm, w1), (w3_hbm, w3), (w2_hbm, w2)))]
    for c in w_copies:
        c.start()
    for s in range(1, hops + 1):
        for d in range(2):
            g_copy(d, s).start()

    def experts(s, gates_t, first, count):
        gates = gates_t.T

        def one(e, _):
            lane = lax.broadcasted_iota(jnp.int32, gates.shape, 1)
            g = jnp.sum(jnp.where(lane == e, gates, 0.0), axis=1, keepdims=True)
            x = ubuf[s]
            f1 = jnp.dot(x, w1[e], preferred_element_type=jnp.float32)
            f3 = jnp.dot(x, w3[e], preferred_element_type=jnp.float32)
            a = (f1 * jax.nn.sigmoid(f1) * f3).astype(jnp.bfloat16)
            width = w2.shape[2]
            for j in range(0, width, 512):
                o = jnp.dot(a, w2[e, :, j:j + 512], preferred_element_type=jnp.float32).astype(jnp.bfloat16).astype(jnp.float32)
                part[s, :, j:j + 512] += jnp.where(g != 0.0, g * o, 0.0)
            return 0

        lax.fori_loop(first, first + count, one, 0)

    for c in loads:
        c.wait()
    for c in w_copies:
        c.wait()
    for s in range(1, hops + 1):
        for d in range(2):
            g_copy(d, s).wait()

    def visit(s, _):
        part[s] = jnp.zeros(part.shape[1:], jnp.float32)

        @pl.when(s == 0)
        def _():
            experts(s, g_ref[lax.rem(pos, g_ref.shape[0])], 0, total)

        @pl.when(s > 0)
        def _():
            for p in range(pieces_u):
                for d in range(2):
                    u_copy(d, s - 1, p).wait_recv()

                    @pl.when(s < hops)
                    def _():
                        u_copy(d, s, p).start()
            experts(s, gbuf[s - 1], 0, total)

        return 0

    lax.fori_loop(0, hops + 1, visit, 0)

    def back(i, _):
        s = hops - i
        for p in range(pieces_a):
            for d in range(2):
                rows = pl.ds(d * half + p * ra, ra)

                @pl.when(i > 0)
                def _():
                    a_copy(d, s + 1, p).wait_recv()
                    part[s, rows] += acc[s, rows]

                @pl.when(s > 0)
                def _():
                    a_copy(d, s, p).start()

                @pl.when(s == 0)
                def _():
                    y_ref[rows] = (h_ref[rows].astype(jnp.float32) + part[s, rows]).astype(y_ref.dtype)
        return 0

    lax.fori_loop(0, hops + 1, back, 0)

    def drain(s, _):
        for d in range(2):
            for p in range(pieces_u):
                u_copy(d, s, p).wait_send()
            for p in range(pieces_a):
                a_copy(d, s + 1, p).wait_send()
        return 0

    lax.fori_loop(0, hops, drain, 0)


def moe(u, gates, hidden, w_one, w_three, w_two, n, hops):
    tok, dim = u.shape
    own, _, ff = w_one.shape
    total = 2 * own
    pieces_u, pieces_a = 2, 4
    dma = pltpu.SemaphoreType.DMA
    any_spec = pl.BlockSpec(memory_space=pl.ANY)
    vmem = pl.BlockSpec(memory_space=pltpu.VMEM)
    return pl.pallas_call(
        functools.partial(moe_kernel, n, hops, pieces_u=pieces_u, pieces_a=pieces_a),
        out_shape=jax.ShapeDtypeStruct((tok, dim), jnp.bfloat16),
        in_specs=[any_spec, vmem, vmem, any_spec, any_spec, any_spec],
        out_specs=vmem,
        scratch_shapes=[
            pltpu.VMEM((hops + 1, tok, dim), jnp.bfloat16),
            pltpu.VMEM((hops, gates.shape[1], tok), jnp.float32),
            pltpu.VMEM((hops + 1, tok, dim), jnp.float32),
            pltpu.VMEM((hops, tok, dim), jnp.float32),
            pltpu.VMEM((total, dim, ff), jnp.bfloat16),
            pltpu.VMEM((total, dim, ff), jnp.bfloat16),
            pltpu.VMEM((total, ff, dim), jnp.bfloat16),
            dma((2, hops, pieces_u)), dma((2, hops, pieces_u)),
            dma((2, hops, pieces_a)), dma((2, hops, pieces_a)),
            dma((2, hops)), dma((2, hops)),
            dma((3,)), dma((3,)), dma((3,)), dma((1,)),
        ],
        compiler_params=pltpu.CompilerParams(collective_id=1, has_side_effects=True, vmem_limit_bytes=66_000_000),
        name='moe_ring',
    )(u, gates, hidden, w_one, w_three, w_two)


def solution(mesh):
    tok_spec = P(('dp', 'ep'))
    row_spec = P('ep')
    n = mesh.shape['ep'] // 2

    def local_layer(tokens, w_query, w_key, w_value, w_out, w_router, w_one, w_three, w_two, expert_ids):
        full_query = lax.all_gather(w_query, 'ep', axis=0, tiled=True)
        full_key = lax.all_gather(w_key, 'ep', axis=0, tiled=True)
        full_value = lax.all_gather(w_value, 'ep', axis=0, tiled=True)
        full_out = lax.all_gather(w_out, 'ep', axis=0, tiled=True)
        hidden = attention_layer(tokens, full_query, full_key, full_value, full_out)
        tok, dim = tokens.shape[0] * tokens.shape[1], tokens.shape[2]
        hidden = hidden.reshape(tok, dim)
        u, gates = router_gates(hidden, w_router, expert_ids.reshape(tok, -1))
        per = gates.shape[0] // n
        gates = jnp.pad(gates.reshape(n, per, tok), ((0, 0), (0, 8 - per), (0, 0)))
        out = moe(u, gates, hidden, w_one, w_three, w_two, n, n - 1)
        return out.reshape(tokens.shape)

    return jax.shard_map(local_layer, mesh=mesh, in_specs=(tok_spec, row_spec, row_spec, row_spec, row_spec, P(), row_spec, row_spec, row_spec, tok_spec), out_specs=tok_spec, check_vma=False)
```

```python
import functools

import jax
import jax.numpy as jnp
from jax import lax
from jax.experimental import pallas as pl
from jax.experimental.pallas import tpu as pltpu
from jax.sharding import PartitionSpec as P

EPS = 1e-6
MESH = pl.DeviceIdType.MESH


def rms_norm(vals):
    wide = vals.astype(jnp.float32)
    return wide * lax.rsqrt(jnp.mean(wide * wide, axis=-1, keepdims=True) + EPS)


def attend_pair(q_ref, k_ref, v_ref, c_ref, i, scale):
    seq, lanes = q_ref.shape[0], 128
    cols = pl.ds(pl.multiple_of(i * lanes, lanes), lanes)
    step = seq // 2
    lane = lax.broadcasted_iota(jnp.int32, (1, lanes), 1)
    keep = [jnp.where(lane < lanes // 2, 1.0, 0.0).astype(jnp.bfloat16), jnp.where(lane < lanes // 2, 0.0, 1.0).astype(jnp.bfloat16)]
    for b in range(2):
        rows, keys = slice(b * step, (b + 1) * step), (b + 1) * step
        q, k, v = q_ref[rows, cols], k_ref[:keys, cols], v_ref[:keys, cols]
        causal = (lax.broadcasted_iota(jnp.int32, (step, keys), 0) + b * step) >= lax.broadcasted_iota(jnp.int32, (step, keys), 1)
        context = None
        for side in range(2):
            s = lax.dot_general(q * keep[side], k, (((1,), (1,)), ((), ())), preferred_element_type=jnp.float32) * scale
            s = jnp.where(causal, s, -jnp.inf)
            e = jnp.exp(s - jnp.max(s, axis=-1, keepdims=True))
            p = (e * (1.0 / jnp.sum(e, axis=-1, keepdims=True))).astype(jnp.bfloat16)
            c = jnp.dot(p, v * keep[side], preferred_element_type=jnp.float32)
            context = c if context is None else context + c
        c_ref[rows, cols] = context.astype(jnp.bfloat16)


def front_kernel(n, head_dim, x_ref, wq_hbm, wk_hbm, wv_hbm, wo_hbm, wr_ref, ids_ref, h_ref, u_ref, g_ref,
                 wbuf, nbuf, qkv, cbuf, r_send, r_recv, d_send, d_recv, loc, *, lag):
    me = lax.axis_index('ep')
    pos, core = lax.div(me, 2), lax.rem(me, 2)
    share = wq_hbm.shape[0]
    half = share // 2
    mats = 4

    def peer(z):
        return {'ep': lax.rem(z + n, n) * 2 + core}

    sibling = {'ep': pos * 2 + (1 - core)}
    barrier = pltpu.get_barrier_semaphore()
    for who in (peer(pos + 1), peer(pos - 1), sibling):
        pl.semaphore_signal(barrier, inc=1, device_id=who, device_id_type=MESH)

    def block(d, s):
        origin = lax.rem(pos + (n - s if d == 0 else s), n) * 2 + core
        return pl.ds(pl.multiple_of(origin * share + d * half, half), half)

    def ring(d, s, m):
        rows = block(d, s)
        return pltpu.make_async_remote_copy(
            src_ref=wbuf.at[m, rows], dst_ref=wbuf.at[m, rows], send_sem=r_send.at[d, s, m], recv_sem=r_recv.at[d, s, m],
            device_id=peer(pos + (1 if d == 0 else n - 1)), device_id_type=MESH)

    def across(d, s, m):
        rows = block(d, s)
        return pltpu.make_async_remote_copy(
            src_ref=wbuf.at[m, rows], dst_ref=wbuf.at[m, rows], send_sem=d_send.at[d, s, m], recv_sem=d_recv.at[d, s, m],
            device_id=sibling, device_id_type=MESH)

    loads = []
    for m, src in enumerate((wq_hbm, wk_hbm, wv_hbm, wo_hbm)):
        loads.append(pltpu.make_async_copy(src, wbuf.at[m, pl.ds(pl.multiple_of(me * share, share), share)], loc.at[m]))
        loads[-1].start()
    pl.semaphore_wait(barrier, 3)
    for m in range(3):
        loads[m].wait()
        for d in range(2):
            ring(d, 0, m).start()
    loads[3].wait()
    for m in range(mats):
        for d in range(2):
            across(d, 0, m).start()
    nbuf[...] = rms_norm(x_ref[...]).astype(jnp.bfloat16)

    def relay(s, m):
        for d in range(2):
            ring(d, s - 1, m).wait_recv()

            @pl.when(s < n - 1)
            def _():
                ring(d, s, m).start()

            across(d, s, m).start()

    def gather(s, _):
        for m in range(3):
            relay(s, m)

        @pl.when(s == lag)
        def _():
            for d in range(2):
                ring(d, 0, 3).start()

        @pl.when(s > lag)
        def _():
            relay(s - lag, 3)

        return 0

    lax.fori_loop(1, n, gather, 0)

    def settle(m0, m1):
        def go(s, _):
            for m in range(m0, m1):
                for d in range(2):
                    across(d, s, m).wait_recv()
            return 0
        lax.fori_loop(0, n, go, 0)

    settle(0, 3)
    width = nbuf.shape[1] // 2

    def project(j, _):
        m, c = lax.div(j, 2), lax.rem(j, 2)
        cols = pl.ds(pl.multiple_of(c * width, width), width)
        qkv[m, :, cols] = jnp.dot(nbuf[...], wbuf[m, :, cols], preferred_element_type=jnp.float32).astype(jnp.bfloat16)
        return 0

    lax.fori_loop(0, 6, project, 0)

    pairs = nbuf.shape[1] // 128
    left = lag

    def heads(i, _):
        attend_pair(qkv.at[0], qkv.at[1], qkv.at[2], cbuf, i, head_dim ** -0.5)

        @pl.when(i < left)
        def _():
            relay(n - lag + i, 3)
        return 0

    lax.fori_loop(0, pairs, heads, 0)
    settle(3, 4)
    for j in range(2):
        cols = slice(j * width, (j + 1) * width)
        mixed = jnp.dot(cbuf[...], wbuf[3, :, cols], preferred_element_type=jnp.float32)
        h_ref[:, cols] = (x_ref[:, cols].astype(jnp.float32) + mixed).astype(jnp.bfloat16)
    z = rms_norm(h_ref[...])
    u_ref[...] = z.astype(jnp.bfloat16)
    logits = lax.dot_general(wr_ref[...], z, (((1,), (1,)), ((), ())), precision=lax.Precision.HIGHEST, preferred_element_type=jnp.float32)
    expert = lax.broadcasted_iota(jnp.int32, logits.shape, 0)
    match = expert == ids_ref[0:1, :]
    for j in range(1, ids_ref.shape[0]):
        match = match | (expert == ids_ref[j:j + 1, :])
    logits = jnp.where(match, logits, -jnp.inf)
    e = jnp.where(match, jnp.exp(logits - jnp.max(logits, axis=0, keepdims=True)), 0.0)
    gates = e / jnp.sum(e, axis=0, keepdims=True)
    classes, rows = g_ref.shape[0], g_ref.shape[1]
    per = gates.shape[0] // n
    for c in range(classes):
        taken = [gates[(c + r * classes) * per:(c + r * classes + 1) * per] for r in range(n // classes)]
        if n // classes * per < rows:
            taken.append(jnp.zeros((rows - n // classes * per, gates.shape[1]), jnp.float32))
        g_ref[c] = jnp.concatenate(taken, axis=0)

    def drain(s, _):
        for m in range(mats):
            for d in range(2):
                across(d, s, m).wait_send()

                @pl.when(s < n - 1)
                def _():
                    ring(d, s, m).wait_send()
        return 0

    lax.fori_loop(0, n, drain, 0)


def front(x, w_query, w_key, w_value, w_out, w_router_t, ids_t, n, classes, head_dim):
    tok, dim = x.shape
    dma = pltpu.SemaphoreType.DMA
    any_spec = pl.BlockSpec(memory_space=pl.ANY)
    vmem = pl.BlockSpec(memory_space=pltpu.VMEM)
    return pl.pallas_call(
        functools.partial(front_kernel, n, head_dim, lag=3),
        out_shape=[jax.ShapeDtypeStruct((tok, dim), jnp.bfloat16), jax.ShapeDtypeStruct((tok, dim), jnp.bfloat16), jax.ShapeDtypeStruct((classes, 8, tok), jnp.float32)],
        in_specs=[vmem, any_spec, any_spec, any_spec, any_spec, vmem, vmem],
        out_specs=[vmem, vmem, vmem],
        scratch_shapes=[
            pltpu.VMEM((4, dim, dim), jnp.bfloat16),
            pltpu.VMEM((tok, dim), jnp.bfloat16),
            pltpu.VMEM((3, tok, dim), jnp.bfloat16),
            pltpu.VMEM((tok, dim), jnp.bfloat16),
            dma((2, n, 4)), dma((2, n, 4)), dma((2, n, 4)), dma((2, n, 4)), dma((4,)),
        ],
        compiler_params=pltpu.CompilerParams(collective_id=2, has_side_effects=True, vmem_limit_bytes=60_000_000),
        name='attention_front',
    )(x, w_query, w_key, w_value, w_out, w_router_t, ids_t)


def moe_kernel(n, hops, u_hbm, g_ref, h_ref, w1_hbm, w3_hbm, w2_hbm, y_ref,
               ubuf, gbuf, part, acc, w1, w3, w2,
               u_send, u_recv, a_send, a_recv, g_send, g_recv, w_send, w_recv, w_loc, u_loc, *, pieces_u, pieces_a):
    me = lax.axis_index('ep')
    pos, core = lax.div(me, 2), lax.rem(me, 2)
    tok, half = ubuf.shape[1], ubuf.shape[1] // 2
    own = w1_hbm.shape[0]
    total = w1.shape[0]
    ru, ra = half // pieces_u, half // pieces_a

    def peer(z):
        return {'ep': lax.rem(z + 2 * n, n) * 2 + core}

    sibling = {'ep': pos * 2 + (1 - core)}

    barrier = pltpu.get_barrier_semaphore()
    for k in range(1, n):
        pl.semaphore_signal(barrier, inc=1, device_id=peer(pos + k), device_id_type=MESH)
    pl.semaphore_signal(barrier, inc=1, device_id=sibling, device_id_type=MESH)

    own_copy = pltpu.make_async_copy(u_hbm, ubuf.at[0], u_loc.at[0])
    own_copy.start()
    mine = pl.ds(core * own, own)
    loads = []
    for i, (src, dst) in enumerate(((w1_hbm, w1), (w3_hbm, w3), (w2_hbm, w2))):
        loads.append(pltpu.make_async_copy(src, dst.at[mine], w_loc.at[i]))
        loads[-1].start()
    pl.semaphore_wait(barrier, n)

    def u_copy(d, s, p):
        rows = pl.ds(d * half + p * ru, ru)
        return pltpu.make_async_remote_copy(
            src_ref=ubuf.at[s, rows], dst_ref=ubuf.at[s + 1, rows],
            send_sem=u_send.at[d, s, p], recv_sem=u_recv.at[d, s, p],
            device_id=peer(pos + (1 if d == 0 else n - 1)), device_id_type=MESH)

    def a_copy(d, s, p):
        rows = pl.ds(d * half + p * ra, ra)
        return pltpu.make_async_remote_copy(
            src_ref=part.at[s, rows], dst_ref=acc.at[s - 1, rows],
            send_sem=a_send.at[d, s - 1, p], recv_sem=a_recv.at[d, s - 1, p],
            device_id=peer(pos + (n - 1 if d == 0 else 1)), device_id_type=MESH)

    def g_copy(d, s):
        cols = pl.ds(d * half, half)
        target = pos + (s if d == 0 else n - s)
        return pltpu.make_async_remote_copy(
            src_ref=g_ref.at[lax.rem(target, g_ref.shape[0]), :, cols], dst_ref=gbuf.at[s - 1, :, cols],
            send_sem=g_send.at[d, s - 1], recv_sem=g_recv.at[d, s - 1],
            device_id=peer(target), device_id_type=MESH)

    def w_copy(i, src, dst):
        return pltpu.make_async_remote_copy(
            src_ref=src, dst_ref=dst.at[mine], send_sem=w_send.at[i], recv_sem=w_recv.at[i],
            device_id=sibling, device_id_type=MESH)

    own_copy.wait()
    for p in range(pieces_u):
        for d in range(2):
            u_copy(d, 0, p).start()
    w_copies = [w_copy(i, s, t) for i, (s, t) in enumerate(((w1_hbm, w1), (w3_hbm, w3), (w2_hbm, w2)))]
    for c in w_copies:
        c.start()
    for s in range(1, hops + 1):
        for d in range(2):
            g_copy(d, s).start()

    def experts(s, gates_t, first, count):
        gates = gates_t.T

        def one(e, _):
            lane = lax.broadcasted_iota(jnp.int32, gates.shape, 1)
            g = jnp.sum(jnp.where(lane == e, gates, 0.0), axis=1, keepdims=True)
            x = ubuf[s]
            f1 = jnp.dot(x, w1[e], preferred_element_type=jnp.float32)
            f3 = jnp.dot(x, w3[e], preferred_element_type=jnp.float32)
            a = (f1 * jax.nn.sigmoid(f1) * f3).astype(jnp.bfloat16)
            width = w2.shape[2]
            for j in range(0, width, 512):
                o = jnp.dot(a, w2[e, :, j:j + 512], preferred_element_type=jnp.float32).astype(jnp.bfloat16).astype(jnp.float32)
                part[s, :, j:j + 512] += jnp.where(g != 0.0, g * o, 0.0)
            return 0

        lax.fori_loop(first, first + count, one, 0)

    for c in loads:
        c.wait()
    for c in w_copies:
        c.wait()
    for s in range(1, hops + 1):
        for d in range(2):
            g_copy(d, s).wait()

    def visit(s, _):
        part[s] = jnp.zeros(part.shape[1:], jnp.float32)

        @pl.when(s == 0)
        def _():
            experts(s, g_ref[lax.rem(pos, g_ref.shape[0])], 0, total)

        @pl.when(s > 0)
        def _():
            for p in range(pieces_u):
                for d in range(2):
                    u_copy(d, s - 1, p).wait_recv()

                    @pl.when(s < hops)
                    def _():
                        u_copy(d, s, p).start()
            experts(s, gbuf[s - 1], 0, total)

        return 0

    lax.fori_loop(0, hops + 1, visit, 0)

    def back(i, _):
        s = hops - i
        for p in range(pieces_a):
            for d in range(2):
                rows = pl.ds(d * half + p * ra, ra)

                @pl.when(i > 0)
                def _():
                    a_copy(d, s + 1, p).wait_recv()
                    part[s, rows] += acc[s, rows]

                @pl.when(s > 0)
                def _():
                    a_copy(d, s, p).start()

                @pl.when(s == 0)
                def _():
                    y_ref[rows] = (h_ref[rows].astype(jnp.float32) + part[s, rows]).astype(y_ref.dtype)
        return 0

    lax.fori_loop(0, hops + 1, back, 0)

    def drain(s, _):
        for d in range(2):
            for p in range(pieces_u):
                u_copy(d, s, p).wait_send()
            for p in range(pieces_a):
                a_copy(d, s + 1, p).wait_send()
        return 0

    lax.fori_loop(0, hops, drain, 0)


def moe(u, gates, hidden, w_one, w_three, w_two, n, hops):
    tok, dim = u.shape
    own, _, ff = w_one.shape
    total = 2 * own
    pieces_u, pieces_a = 2, 4
    dma = pltpu.SemaphoreType.DMA
    any_spec = pl.BlockSpec(memory_space=pl.ANY)
    vmem = pl.BlockSpec(memory_space=pltpu.VMEM)
    return pl.pallas_call(
        functools.partial(moe_kernel, n, hops, pieces_u=pieces_u, pieces_a=pieces_a),
        out_shape=jax.ShapeDtypeStruct((tok, dim), jnp.bfloat16),
        in_specs=[any_spec, vmem, vmem, any_spec, any_spec, any_spec],
        out_specs=vmem,
        scratch_shapes=[
            pltpu.VMEM((hops + 1, tok, dim), jnp.bfloat16),
            pltpu.VMEM((hops, gates.shape[1], tok), jnp.float32),
            pltpu.VMEM((hops + 1, tok, dim), jnp.float32),
            pltpu.VMEM((hops, tok, dim), jnp.float32),
            pltpu.VMEM((total, dim, ff), jnp.bfloat16),
            pltpu.VMEM((total, dim, ff), jnp.bfloat16),
            pltpu.VMEM((total, ff, dim), jnp.bfloat16),
            dma((2, hops, pieces_u)), dma((2, hops, pieces_u)),
            dma((2, hops, pieces_a)), dma((2, hops, pieces_a)),
            dma((2, hops)), dma((2, hops)),
            dma((3,)), dma((3,)), dma((3,)), dma((1,)),
        ],
        compiler_params=pltpu.CompilerParams(collective_id=1, has_side_effects=True, vmem_limit_bytes=66_000_000),
        name='moe_ring',
    )(u, gates, hidden, w_one, w_three, w_two)


def solution(mesh):
    tok_spec = P(('dp', 'ep'))
    row_spec = P('ep')
    n = mesh.shape['ep'] // 2

    def local_layer(tokens, w_query, w_key, w_value, w_out, w_router, w_one, w_three, w_two, expert_ids):
        tok, dim = tokens.shape[0] * tokens.shape[1], tokens.shape[2]
        flat = [w.reshape(w.shape[0], -1) for w in (w_query, w_key, w_value)]
        ids_t = expert_ids.reshape(tok, -1).T
        hidden, u, gates = front(tokens.reshape(tok, dim), *flat, w_out, w_router.T, ids_t, n, n, w_query.shape[2])
        out = moe(u, gates, hidden, w_one, w_three, w_two, n, n - 1)
        return out.reshape(tokens.shape)

    return jax.shard_map(local_layer, mesh=mesh, in_specs=(tok_spec, row_spec, row_spec, row_spec, row_spec, P(), row_spec, row_spec, row_spec, tok_spec), out_specs=tok_spec, check_vma=False)
```

```python
import functools

import jax
import jax.numpy as jnp
from jax import lax
from jax.experimental import pallas as pl
from jax.experimental.pallas import tpu as pltpu
from jax.sharding import PartitionSpec as P

EPS = 1e-6
MESH = pl.DeviceIdType.MESH


def rms_norm(vals):
    wide = vals.astype(jnp.float32)
    return wide * lax.rsqrt(jnp.mean(wide * wide, axis=-1, keepdims=True) + EPS)


def attend_pair(q_ref, k_ref, v_ref, c_ref, i, scale):
    seq, lanes = q_ref.shape[0], 128
    cols = pl.ds(pl.multiple_of(i * lanes, lanes), lanes)
    step = seq // 2
    lane = lax.broadcasted_iota(jnp.int32, (1, lanes), 1)
    keep = [jnp.where(lane < lanes // 2, 1.0, 0.0).astype(jnp.bfloat16), jnp.where(lane < lanes // 2, 0.0, 1.0).astype(jnp.bfloat16)]
    for b in range(2):
        rows, keys = slice(b * step, (b + 1) * step), (b + 1) * step
        q, k, v = q_ref[rows, cols], k_ref[:keys, cols], v_ref[:keys, cols]
        causal = (lax.broadcasted_iota(jnp.int32, (step, keys), 0) + b * step) >= lax.broadcasted_iota(jnp.int32, (step, keys), 1)
        context = None
        for side in range(2):
            s = lax.dot_general(q * keep[side], k, (((1,), (1,)), ((), ())), preferred_element_type=jnp.float32) * scale
            s = jnp.where(causal, s, -jnp.inf)
            e = jnp.exp(s - jnp.max(s, axis=-1, keepdims=True))
            p = (e * (1.0 / jnp.sum(e, axis=-1, keepdims=True))).astype(jnp.bfloat16)
            c = jnp.dot(p, v * keep[side], preferred_element_type=jnp.float32)
            context = c if context is None else context + c
        c_ref[rows, cols] = context.astype(jnp.bfloat16)


def front_kernel(n, groups, head_dim, x_ref, wq_hbm, wk_hbm, wv_hbm, wo_hbm, wr_ref, ids_ref, e1_hbm, e3_hbm, e2_hbm,
                 h_ref, u_ref, g_ref, f1_hbm, f3_hbm, f2_hbm,
                 wbuf, nbuf, qkv, cbuf, mid1, mid3, mid2, r_send, r_recv, d_send, d_recv, loc,
                 s1_send, s1_recv, s2_send, s2_recv, s3_send, s3_recv, *, lag):
    me = lax.axis_index('ep')
    pos, core = lax.div(me, 2), lax.rem(me, 2)
    share = wq_hbm.shape[0]
    half = share // 2
    mats = 4

    def peer(z):
        return {'ep': lax.rem(z + n, n) * 2 + core}

    sibling = {'ep': pos * 2 + (1 - core)}
    barrier = pltpu.get_barrier_semaphore()
    for who in (peer(pos + 1), peer(pos + n - 1), peer(pos + 2), peer(pos + n - 2), sibling):
        pl.semaphore_signal(barrier, inc=1, device_id=who, device_id_type=MESH)
    group = lax.axis_index('dp')

    def other(j):
        return {'dp': lax.rem(group + j, groups)}

    def greet(j, _):
        pl.semaphore_signal(barrier, inc=1, device_id=other(j), device_id_type=MESH)
        return 0

    lax.fori_loop(1, groups, greet, 0)
    far = ((e1_hbm, mid1, f1_hbm), (e3_hbm, mid3, f3_hbm), (e2_hbm, mid2, f2_hbm))

    def part_rows(t, d):
        size = far[t][0].shape[1] // (2 * groups)
        return pl.ds(pl.multiple_of((group * 2 + d) * size, size), size)

    def stage(t, d, k):
        own, mid, out = far[t]
        rows = part_rows(t, d)
        two = peer(pos + (2 if d == 0 else n - 2))
        if k == 1:
            return pltpu.make_async_remote_copy(src_ref=own.at[:, rows], dst_ref=mid.at[d], send_sem=s1_send.at[t, d], recv_sem=s1_recv.at[t, d], device_id=two, device_id_type=MESH)
        return pltpu.make_async_remote_copy(src_ref=mid.at[d], dst_ref=out.at[:, rows], send_sem=s2_send.at[t, d], recv_sem=s2_recv.at[t, d], device_id=two, device_id_type=MESH)

    def spread(t, d, j):
        out, rows = far[t][2], part_rows(t, d)
        return pltpu.make_async_remote_copy(src_ref=out.at[:, rows], dst_ref=out.at[:, rows], send_sem=s3_send.at[t, d, j - 1], recv_sem=s3_recv.at[t, d, j - 1], device_id=other(j), device_id_type=MESH)

    def onward(t):
        for d in range(2):
            stage(t, d, 1).wait_recv()
            stage(t, d, 2).start()

    def share_out(t):
        for d in range(2):
            stage(t, d, 2).wait_recv()

            def send(j, _):
                spread(t, d, j).start()
                return 0

            lax.fori_loop(1, groups, send, 0)

    def block(d, s):
        origin = lax.rem(pos + (n - s if d == 0 else s), n) * 2 + core
        return pl.ds(pl.multiple_of(origin * share + d * half, half), half)

    def ring(d, s, m):
        rows = block(d, s)
        return pltpu.make_async_remote_copy(
            src_ref=wbuf.at[m, rows], dst_ref=wbuf.at[m, rows], send_sem=r_send.at[d, s, m], recv_sem=r_recv.at[d, s, m],
            device_id=peer(pos + (1 if d == 0 else n - 1)), device_id_type=MESH)

    def across(d, s, m):
        rows = block(d, s)
        return pltpu.make_async_remote_copy(
            src_ref=wbuf.at[m, rows], dst_ref=wbuf.at[m, rows], send_sem=d_send.at[d, s, m], recv_sem=d_recv.at[d, s, m],
            device_id=sibling, device_id_type=MESH)

    loads = []
    for m, src in enumerate((wq_hbm, wk_hbm, wv_hbm, wo_hbm)):
        loads.append(pltpu.make_async_copy(src, wbuf.at[m, pl.ds(pl.multiple_of(me * share, share), share)], loc.at[m]))
        loads[-1].start()
    pl.semaphore_wait(barrier, 4 + groups)
    for m in range(3):
        loads[m].wait()
        for d in range(2):
            ring(d, 0, m).start()
    loads[3].wait()
    for m in range(mats):
        for d in range(2):
            across(d, 0, m).start()
    nbuf[...] = rms_norm(x_ref[...]).astype(jnp.bfloat16)

    def relay(s, m):
        for d in range(2):
            ring(d, s - 1, m).wait_recv()

            @pl.when(s < n - 1)
            def _():
                ring(d, s, m).start()

            across(d, s, m).start()

    def gather(s, _):
        for m in range(3):
            relay(s, m)

        @pl.when(s == lag)
        def _():
            for d in range(2):
                ring(d, 0, 3).start()

        @pl.when(s > lag)
        def _():
            relay(s - lag, 3)

        return 0

    lax.fori_loop(1, n, gather, 0)

    def settle(m0, m1):
        def go(s, _):
            for m in range(m0, m1):
                for d in range(2):
                    across(d, s, m).wait_recv()
            return 0
        lax.fori_loop(0, n, go, 0)

    for t in range(3):
        for d in range(2):
            stage(t, d, 1).start()
    settle(0, 3)
    width = nbuf.shape[1] // 2

    def project(j, _):
        m, c = lax.div(j, 2), lax.rem(j, 2)
        cols = pl.ds(pl.multiple_of(c * width, width), width)
        qkv[m, :, cols] = jnp.dot(nbuf[...], wbuf[m, :, cols], preferred_element_type=jnp.float32).astype(jnp.bfloat16)
        return 0

    lax.fori_loop(0, 6, project, 0)

    pairs = nbuf.shape[1] // 128
    left = lag

    def heads(i, _):
        attend_pair(qkv.at[0], qkv.at[1], qkv.at[2], cbuf, i, head_dim ** -0.5)

        @pl.when(i < left)
        def _():
            relay(n - lag + i, 3)

        @pl.when(i == pairs // 2)
        def _():
            onward(0)
        return 0

    lax.fori_loop(0, pairs, heads, 0)
    settle(3, 4)
    onward(1)
    for j in range(2):
        cols = slice(j * width, (j + 1) * width)
        mixed = jnp.dot(cbuf[...], wbuf[3, :, cols], preferred_element_type=jnp.float32)
        h_ref[:, cols] = (x_ref[:, cols].astype(jnp.float32) + mixed).astype(jnp.bfloat16)
    z = rms_norm(h_ref[...])
    u_ref[...] = z.astype(jnp.bfloat16)
    logits = lax.dot_general(wr_ref[...], z, (((1,), (1,)), ((), ())), precision=lax.Precision.HIGHEST, preferred_element_type=jnp.float32)
    expert = lax.broadcasted_iota(jnp.int32, logits.shape, 0)
    match = expert == ids_ref[0:1, :]
    for j in range(1, ids_ref.shape[0]):
        match = match | (expert == ids_ref[j:j + 1, :])
    logits = jnp.where(match, logits, -jnp.inf)
    e = jnp.where(match, jnp.exp(logits - jnp.max(logits, axis=0, keepdims=True)), 0.0)
    gates = e / jnp.sum(e, axis=0, keepdims=True)
    classes, rows = g_ref.shape[0], g_ref.shape[1]
    per = gates.shape[0] // n
    for c in range(classes):
        taken = [gates[(c + r * classes) * per:(c + r * classes + 1) * per] for r in range(n // classes)]
        if n // classes * per < rows:
            taken.append(jnp.zeros((rows - n // classes * per, gates.shape[1]), jnp.float32))
        g_ref[c] = jnp.concatenate(taken, axis=0)
    onward(2)
    for t in range(3):
        share_out(t)

    def finish(j, _):
        for t in range(3):
            for d in range(2):
                spread(t, d, j).wait()
        return 0

    lax.fori_loop(1, groups, finish, 0)
    for t in range(3):
        for d in range(2):
            stage(t, d, 1).wait_send()
            stage(t, d, 2).wait_send()

    def drain(s, _):
        for m in range(mats):
            for d in range(2):
                across(d, s, m).wait_send()

                @pl.when(s < n - 1)
                def _():
                    ring(d, s, m).wait_send()
        return 0

    lax.fori_loop(0, n, drain, 0)


def front(x, w_query, w_key, w_value, w_out, w_router_t, ids_t, w_one, w_three, w_two, n, groups, classes, head_dim):
    tok, dim = x.shape
    dma = pltpu.SemaphoreType.DMA
    any_spec = pl.BlockSpec(memory_space=pl.ANY)
    vmem = pl.BlockSpec(memory_space=pltpu.VMEM)
    return pl.pallas_call(
        functools.partial(front_kernel, n, groups, head_dim, lag=3),
        out_shape=[jax.ShapeDtypeStruct((tok, dim), jnp.bfloat16), jax.ShapeDtypeStruct((tok, dim), jnp.bfloat16), jax.ShapeDtypeStruct((classes, 8, tok), jnp.float32),
                   *(jax.ShapeDtypeStruct(w.shape, w.dtype) for w in (w_one, w_three, w_two))],
        in_specs=[vmem, any_spec, any_spec, any_spec, any_spec, vmem, vmem, any_spec, any_spec, any_spec],
        out_specs=[vmem, vmem, vmem, any_spec, any_spec, any_spec],
        scratch_shapes=[
            pltpu.VMEM((4, dim, dim), jnp.bfloat16),
            pltpu.VMEM((tok, dim), jnp.bfloat16),
            pltpu.VMEM((3, tok, dim), jnp.bfloat16),
            pltpu.VMEM((tok, dim), jnp.bfloat16),
            *(pltpu.VMEM((2, w.shape[0], w.shape[1] // (2 * groups), w.shape[2]), jnp.bfloat16) for w in (w_one, w_three, w_two)),
            dma((2, n, 4)), dma((2, n, 4)), dma((2, n, 4)), dma((2, n, 4)), dma((4,)),
            dma((3, 2)), dma((3, 2)), dma((3, 2)), dma((3, 2)), dma((3, 2, groups - 1)), dma((3, 2, groups - 1)),
        ],
        compiler_params=pltpu.CompilerParams(collective_id=2, has_side_effects=True, vmem_limit_bytes=60_000_000),
        name='attention_front',
    )(x, w_query, w_key, w_value, w_out, w_router_t, ids_t, w_one, w_three, w_two)


def moe_kernel(n, hops, u_hbm, g_ref, h_ref, w1_hbm, w3_hbm, w2_hbm, f1_hbm, f3_hbm, f2_hbm, y_ref,
               ubuf, gbuf, part, acc, w1, w3, w2,
               u_send, u_recv, a_send, a_recv, g_send, g_recv, w_send, w_recv, w_loc, u_loc, *, pieces_u, pieces_a):
    me = lax.axis_index('ep')
    pos, core = lax.div(me, 2), lax.rem(me, 2)
    tok = ubuf.shape[1]
    own = w1_hbm.shape[0]
    classes = g_ref.shape[0]
    ru = tok // (2 * pieces_u)
    per = pieces_a // pieces_u
    ra = ru // per

    def peer(z):
        return {'ep': lax.rem(z + 2 * n, n) * 2 + core}

    sibling = {'ep': pos * 2 + (1 - core)}

    barrier = pltpu.get_barrier_semaphore()
    for k in range(1, hops + 1):
        pl.semaphore_signal(barrier, inc=1, device_id=peer(pos + k), device_id_type=MESH)
        pl.semaphore_signal(barrier, inc=1, device_id=peer(pos + n - k), device_id_type=MESH)
    pl.semaphore_signal(barrier, inc=1, device_id=sibling, device_id_type=MESH)

    own_copy = pltpu.make_async_copy(u_hbm, ubuf.at[0], u_loc.at[0])
    own_copy.start()
    near, away = lax.div(pos, classes) * 2 * own, (1 - lax.div(pos, classes)) * 2 * own
    base = [near + core * own, away + core * own, near + (1 - core) * own, away + (1 - core) * own]
    mats = ((w1_hbm, f1_hbm, w1), (w3_hbm, f3_hbm, w3), (w2_hbm, f2_hbm, w2))

    def load(r, i):
        return pltpu.make_async_copy(mats[i][r], mats[i][2].at[pl.ds(base[r], own)], w_loc.at[r, i])

    def hand(r, i):
        return pltpu.make_async_remote_copy(
            src_ref=mats[i][r], dst_ref=mats[i][2].at[pl.ds(base[r], own)], send_sem=w_send.at[r, i], recv_sem=w_recv.at[r, i],
            device_id=sibling, device_id_type=MESH)

    for r in range(2):
        for i in range(3):
            load(r, i).start()
    pl.semaphore_wait(barrier, 2 * hops + 1)

    def u_copy(d, s, p):
        rows = pl.ds((2 * p + d) * ru, ru)
        return pltpu.make_async_remote_copy(
            src_ref=ubuf.at[s, rows], dst_ref=ubuf.at[s + 1, rows],
            send_sem=u_send.at[d, s, p], recv_sem=u_recv.at[d, s, p],
            device_id=peer(pos + (1 if d == 0 else n - 1)), device_id_type=MESH)

    def a_rows(d, p):
        return pl.ds((2 * (p // per) + d) * ru + (p % per) * ra, ra)

    def a_copy(d, s, p):
        rows = a_rows(d, p)
        return pltpu.make_async_remote_copy(
            src_ref=part.at[s, rows], dst_ref=acc.at[s - 1, rows],
            send_sem=a_send.at[d, s - 1, p], recv_sem=a_recv.at[d, s - 1, p],
            device_id=peer(pos + (n - 1 if d == 0 else 1)), device_id_type=MESH)

    def g_copy(d, s):
        target = pos + (s if d == 0 else n - s)
        return pltpu.make_async_remote_copy(
            src_ref=g_ref.at[lax.rem(target, classes)], dst_ref=gbuf.at[d, s - 1],
            send_sem=g_send.at[d, s - 1], recv_sem=g_recv.at[d, s - 1],
            device_id=peer(target), device_id_type=MESH)

    own_copy.wait()
    for p in range(pieces_u):
        for d in range(2):
            u_copy(d, 0, p).start()
    for r in range(2):
        for i in range(3):
            hand(r, i).start()
    for s in range(1, hops + 1):
        for d in range(2):
            g_copy(d, s).start()

    def experts(s, gates, first, count, start, rows):
        here = slice(start, start + rows)
        gates = gates.T[here]

        def one(e, fresh):
            turn = lax.div(e, own)
            slot = jnp.where(turn == 0, base[0], jnp.where(turn == 1, base[1], jnp.where(turn == 2, base[2], base[3]))) + lax.rem(e, own)
            lane = lax.broadcasted_iota(jnp.int32, gates.shape, 1)
            g = jnp.sum(jnp.where(lane == slot, gates, 0.0), axis=1, keepdims=True)
            x = ubuf[s, here]
            f1 = jnp.dot(x, w1[slot], preferred_element_type=jnp.float32)
            f3 = jnp.dot(x, w3[slot], preferred_element_type=jnp.float32)
            a = (f1 * jax.nn.sigmoid(f1) * f3).astype(jnp.bfloat16)
            width = w2.shape[2]
            for j in range(0, width, 512):
                o = jnp.dot(a, w2[slot, :, j:j + 512], preferred_element_type=jnp.float32).astype(jnp.bfloat16).astype(jnp.float32)
                part[s, here, j:j + 512] += jnp.where(g != 0.0, g * o, 0.0)
            return 0

        lax.fori_loop(first, first + count, one, 0)

    def gates_of(s):
        lane = lax.broadcasted_iota(jnp.int32, gbuf.shape[2:], 1)
        return jnp.where(lax.rem(lax.div(lane, ru), 2) == 0, gbuf[0, s - 1], gbuf[1, s - 1])

    def forward(s):
        for p in range(pieces_u):
            for d in range(2):
                u_copy(d, s - 1, p).wait_recv()
                if s < hops:
                    u_copy(d, s, p).start()

    for s in range(hops + 1):
        part[s] = jnp.zeros(part.shape[1:], jnp.float32)
    mine = g_ref[lax.rem(pos, classes)]
    for i in range(3):
        load(0, i).wait()
    experts(0, mine, 0, own, 0, tok)
    for i in range(3):
        load(1, i).wait()
    experts(0, mine, own, own, 0, tok)
    forward(1)
    for r in range(2):
        for i in range(3):
            hand(r, i).wait()
    experts(0, mine, 2 * own, 2 * own, 0, tok)
    for s in range(1, hops + 1):
        for d in range(2):
            g_copy(d, s).wait()
    forward(2)
    experts(1, gates_of(1), 0, 4 * own, 0, tok)
    for s in range(3, hops + 1):
        forward(s)
    last = gates_of(hops)
    for p in range(pieces_u):
        experts(hops, last, 0, 4 * own, p * 2 * ru, 2 * ru)
        for q in range(p * per, (p + 1) * per):
            for d in range(2):
                a_copy(d, hops, q).start()
    for s in range(hops - 1, 1, -1):
        experts(s, gates_of(s), 0, 4 * own, 0, tok)

    for s in range(hops - 1, -1, -1):
        for p in range(pieces_a):
            for d in range(2):
                rows = a_rows(d, p)
                a_copy(d, s + 1, p).wait_recv()
                if s > 0:
                    part[s, rows] += acc[s, rows]
                    a_copy(d, s, p).start()
                else:
                    y_ref[rows] = (h_ref[rows].astype(jnp.float32) + (part[s, rows] + acc[s, rows])).astype(y_ref.dtype)

    for s in range(hops):
        for d in range(2):
            for p in range(pieces_u):
                u_copy(d, s, p).wait_send()
            for p in range(pieces_a):
                a_copy(d, s + 1, p).wait_send()


def moe(u, gates, hidden, w_one, w_three, w_two, far, n):
    tok, dim = u.shape
    own, _, ff = w_one.shape
    classes = gates.shape[0]
    hops, total = classes - 1, 2 * own * (n // classes)
    pieces_u, pieces_a = 2, 4
    dma = pltpu.SemaphoreType.DMA
    any_spec = pl.BlockSpec(memory_space=pl.ANY)
    vmem = pl.BlockSpec(memory_space=pltpu.VMEM)
    return pl.pallas_call(
        functools.partial(moe_kernel, n, hops, pieces_u=pieces_u, pieces_a=pieces_a),
        out_shape=jax.ShapeDtypeStruct((tok, dim), jnp.bfloat16),
        in_specs=[any_spec, vmem, vmem] + [any_spec] * 6,
        out_specs=vmem,
        scratch_shapes=[
            pltpu.VMEM((hops + 1, tok, dim), jnp.bfloat16),
            pltpu.VMEM((2, hops, gates.shape[1], tok), jnp.float32),
            pltpu.VMEM((hops + 1, tok, dim), jnp.float32),
            pltpu.VMEM((hops, tok, dim), jnp.float32),
            pltpu.VMEM((total, dim, ff), jnp.bfloat16),
            pltpu.VMEM((total, dim, ff), jnp.bfloat16),
            pltpu.VMEM((total, ff, dim), jnp.bfloat16),
            dma((2, hops, pieces_u)), dma((2, hops, pieces_u)),
            dma((2, hops, pieces_a)), dma((2, hops, pieces_a)),
            dma((2, hops)), dma((2, hops)),
            dma((2, 3)), dma((2, 3)), dma((2, 3)), dma((1,)),
        ],
        compiler_params=pltpu.CompilerParams(collective_id=1, has_side_effects=True, vmem_limit_bytes=66_000_000),
        name='moe_ring',
    )(u, gates, hidden, w_one, w_three, w_two, *far)


def solution(mesh):
    tok_spec = P(('dp', 'ep'))
    row_spec = P('ep')
    n = mesh.shape['ep'] // 2
    groups = mesh.shape['dp']

    def local_layer(tokens, w_query, w_key, w_value, w_out, w_router, w_one, w_three, w_two, expert_ids):
        tok, dim = tokens.shape[0] * tokens.shape[1], tokens.shape[2]
        flat = [w.reshape(w.shape[0], -1) for w in (w_query, w_key, w_value)]
        ids_t = expert_ids.reshape(tok, -1).T
        hidden, u, gates, *far = front(tokens.reshape(tok, dim), *flat, w_out, w_router.T, ids_t, w_one, w_three, w_two, n, groups, n // 2, w_query.shape[2])
        out = moe(u, gates, hidden, w_one, w_three, w_two, far, n)
        return out.reshape(tokens.shape)

    return jax.shard_map(local_layer, mesh=mesh, in_specs=(tok_spec, row_spec, row_spec, row_spec, row_spec, P(), row_spec, row_spec, row_spec, tok_spec), out_specs=tok_spec, check_vma=False)
```

```python
import functools

import jax
import jax.numpy as jnp
from jax import lax
from jax.experimental import pallas as pl
from jax.experimental.pallas import tpu as pltpu
from jax.sharding import PartitionSpec as P

EPS = 1e-6
MESH = pl.DeviceIdType.MESH


def rms_norm(vals):
    wide = vals.astype(jnp.float32)
    return wide * lax.rsqrt(jnp.mean(wide * wide, axis=-1, keepdims=True) + EPS)


def attend_pair(q_ref, k_ref, v_ref, c_ref, i, scale):
    seq, lanes = q_ref.shape[0], 128
    cols = pl.ds(pl.multiple_of(i * lanes, lanes), lanes)
    step = seq // 2
    lane = lax.broadcasted_iota(jnp.int32, (1, lanes), 1)
    keep = [jnp.where(lane < lanes // 2, 1.0, 0.0).astype(jnp.bfloat16), jnp.where(lane < lanes // 2, 0.0, 1.0).astype(jnp.bfloat16)]
    for b in range(2):
        rows, keys = slice(b * step, (b + 1) * step), (b + 1) * step
        q, k, v = q_ref[rows, cols], k_ref[:keys, cols], v_ref[:keys, cols]
        causal = (lax.broadcasted_iota(jnp.int32, (step, keys), 0) + b * step) >= lax.broadcasted_iota(jnp.int32, (step, keys), 1)
        context = None
        for side in range(2):
            s = lax.dot_general(q * keep[side], k, (((1,), (1,)), ((), ())), preferred_element_type=jnp.float32) * scale
            s = jnp.where(causal, s, -jnp.inf)
            e = jnp.exp(s - jnp.max(s, axis=-1, keepdims=True))
            p = (e * (1.0 / jnp.sum(e, axis=-1, keepdims=True))).astype(jnp.bfloat16)
            c = jnp.dot(p, v * keep[side], preferred_element_type=jnp.float32)
            context = c if context is None else context + c
        c_ref[rows, cols] = context.astype(jnp.bfloat16)


def layer_kernel(n, groups, head_dim, x_ref, wq_hbm, wk_hbm, wv_hbm, wo_hbm, wr_ref, ids_ref, e1_hbm, e3_hbm, e2_hbm, y_ref,
                 wbuf, nbuf, qkv, ubuf, g_own, gbuf, part, acc, w1, w3, w2,
                 r_send, r_recv, d_send, d_recv, loc, w_loc, z_send, z_recv, s_send, s_recv, w_send, w_recv,
                 u_send, u_recv, a_send, a_recv, g_send, g_recv, *, pieces_u, pieces_a):
    me, group = lax.axis_index('ep'), lax.axis_index('dp')
    pos, core = lax.div(me, 2), lax.rem(me, 2)
    share = wq_hbm.shape[0]
    half = share // 2
    mats = 4
    tok, dim = x_ref.shape
    own, classes = e1_hbm.shape[0], g_own.shape[0]
    hops = classes - 1
    ru = tok // (2 * pieces_u)
    per = pieces_a // pieces_u
    ra = ru // per

    def peer(z):
        return {'ep': lax.rem(z, n) * 2 + core}

    def other(j):
        return {'dp': lax.rem(group + j, groups)}

    sibling = {'ep': pos * 2 + (1 - core)}

    def remote(src, dst, send, recv, device):
        return pltpu.make_async_remote_copy(src_ref=src, dst_ref=dst, send_sem=send, recv_sem=recv, device_id=device, device_id_type=MESH)

    barrier = pltpu.get_barrier_semaphore()

    def greet_ring(k, _):
        pl.semaphore_signal(barrier, inc=1, device_id=peer(pos + k), device_id_type=MESH)
        return 0

    def greet_groups(j, _):
        pl.semaphore_signal(barrier, inc=1, device_id=other(j), device_id_type=MESH)
        return 0

    lax.fori_loop(1, n, greet_ring, 0)
    lax.fori_loop(1, groups, greet_groups, 0)
    pl.semaphore_signal(barrier, inc=1, device_id=sibling, device_id_type=MESH)


    def block(d, s):
        origin = lax.rem(pos + (n - s if d == 0 else s), n) * 2 + core
        return pl.ds(pl.multiple_of(origin * share + d * half, half), half)

    def ring(d, s, m):
        rows = block(d, s)
        return remote(wbuf.at[m, rows], wbuf.at[m, rows], r_send.at[d, s, m], r_recv.at[d, s, m], peer(pos + (1 if d == 0 else n - 1)))

    def across(d, s, m):
        rows = block(d, s)
        return remote(wbuf.at[m, rows], wbuf.at[m, rows], d_send.at[d, s, m], d_recv.at[d, s, m], sibling)


    near, away = lax.div(pos, classes) * 2 * own, (1 - lax.div(pos, classes)) * 2 * own
    base = [near + core * own, near + (1 - core) * own, away + core * own, away + (1 - core) * own]
    experts_of = ((e1_hbm, w1), (e3_hbm, w3), (e2_hbm, w2))

    def rows_of(t, d):
        size = experts_of[t][0].shape[1] // (2 * groups)
        return pl.ds(pl.multiple_of((group * 2 + d) * size, size), size)

    def load(t):
        return pltpu.make_async_copy(experts_of[t][0], experts_of[t][1].at[pl.ds(base[0], own)], w_loc.at[t])

    def hand(r, t):
        kept = experts_of[t][1].at[pl.ds(base[2 * r], own)]
        return remote(experts_of[t][0] if r == 0 else kept, kept, w_send.at[r, t], w_recv.at[r, t], sibling)

    def fetch(t, d):
        rows = rows_of(t, d)
        return remote(experts_of[t][0].at[:, rows], experts_of[t][1].at[pl.ds(base[0], own), rows], z_send.at[t, d], z_recv.at[t, d], peer(pos + n // 2))

    def spread(t, d, j):
        piece = experts_of[t][1].at[pl.ds(base[2], own), rows_of(t, d)]
        return remote(piece, piece, s_send.at[t, d, j - 1], s_recv.at[t, d, j - 1], other(j))

    def share_out(t, d):
        fetch(t, d).wait_recv()

        def send(j, _):
            spread(t, d, j).start()
            return 0

        lax.fori_loop(1, groups, send, 0)

    def collect(t):
        def take(j, _):
            for d in range(2):
                spread(t, d, j).wait_recv()
            return 0

        lax.fori_loop(1, groups, take, 0)
        hand(1, t).start()

    shards = []
    for m, src in enumerate((wq_hbm, wk_hbm, wv_hbm, wo_hbm)):
        shards.append(pltpu.make_async_copy(src, wbuf.at[m, pl.ds(pl.multiple_of(me * share, share), share)], loc.at[m]))
        shards[-1].start()
    for t in range(3):
        load(t).start()
    pl.semaphore_wait(barrier, n + groups - 1)
    for m in range(mats):
        shards[m].wait()
        for d in range(2):
            ring(d, 0, m).start()
    for m in range(mats):
        for d in range(2):
            across(d, 0, m).start()
    for t in range(3):
        hand(0, t).start()
    nbuf[...] = rms_norm(x_ref[...]).astype(jnp.bfloat16)
    for s in range(hops + 1):
        part[s] = jnp.zeros(part.shape[1:], jnp.float32)

    def gather(s, _):
        for m in range(mats):
            for d in range(2):
                ring(d, s - 1, m).wait_recv()

                @pl.when(s < n - 1)
                def _():
                    ring(d, s, m).start()

                across(d, s, m).start()
        return 0

    lax.fori_loop(1, n, gather, 0)
    for t in range(3):
        for d in range(2):
            fetch(t, d).start()

    def settle(s, _):
        for m in range(mats):
            for d in range(2):
                across(d, s, m).wait_recv()
        return 0

    lax.fori_loop(0, n, settle, 0)
    width = dim // 2

    def project(j, _):
        m, c = lax.div(j, 2), lax.rem(j, 2)
        cols = pl.ds(pl.multiple_of(c * width, width), width)
        qkv[m, :, cols] = jnp.dot(nbuf[...], wbuf[m, :, cols], preferred_element_type=jnp.float32).astype(jnp.bfloat16)
        return 0

    lax.fori_loop(0, 6, project, 0)
    pairs = dim // 128

    def heads(i, _):
        attend_pair(qkv.at[0], qkv.at[1], qkv.at[2], nbuf, i, head_dim ** -0.5)

        @pl.when(i == pairs // 2)
        def _():
            share_out(0, 0)
        return 0

    lax.fori_loop(0, pairs, heads, 0)
    share_out(0, 1)
    for j in range(2):
        cols = slice(j * width, (j + 1) * width)
        mixed = jnp.dot(nbuf[...], wbuf[3, :, cols], preferred_element_type=jnp.float32)
        y_ref[:, cols] = (x_ref[:, cols].astype(jnp.float32) + mixed).astype(jnp.bfloat16)
    z = rms_norm(y_ref[...])
    ubuf[0] = z.astype(jnp.bfloat16)
    logits = lax.dot_general(wr_ref[...], z, (((1,), (1,)), ((), ())), precision=lax.Precision.HIGHEST, preferred_element_type=jnp.float32)
    expert = lax.broadcasted_iota(jnp.int32, logits.shape, 0)
    match = expert == ids_ref[0:1, :]
    for j in range(1, ids_ref.shape[0]):
        match = match | (expert == ids_ref[j:j + 1, :])
    logits = jnp.where(match, logits, -jnp.inf)
    e = jnp.where(match, jnp.exp(logits - jnp.max(logits, axis=0, keepdims=True)), 0.0)
    gates = e / jnp.sum(e, axis=0, keepdims=True)
    layer = gates.shape[0] // n
    for c in range(classes):
        g_own[c] = jnp.concatenate([gates[(c + r * classes) * layer:(c + r * classes + 1) * layer] for r in range(n // classes)], axis=0)


    def u_copy(d, s, p):
        rows = pl.ds((2 * p + d) * ru, ru)
        return remote(ubuf.at[s, rows], ubuf.at[s + 1, rows], u_send.at[d, s, p], u_recv.at[d, s, p], peer(pos + (1 if d == 0 else n - 1)))

    def a_rows(d, p):
        return pl.ds((2 * (p // per) + d) * ru + (p % per) * ra, ra)

    def a_copy(d, s, p):
        rows = a_rows(d, p)
        return remote(part.at[s, rows], acc.at[s - 1, rows], a_send.at[d, s - 1, p], a_recv.at[d, s - 1, p], peer(pos + (n - 1 if d == 0 else 1)))

    def g_copy(d, s):
        target = pos + (s if d == 0 else n - s)
        return remote(g_own.at[lax.rem(target, classes)], gbuf.at[d, s - 1], g_send.at[d, s - 1], g_recv.at[d, s - 1], peer(target))

    for p in range(pieces_u):
        for d in range(2):
            u_copy(d, 0, p).start()

    def experts(s, gates, first, count, start=0, rows=tok):
        here = slice(start, start + rows)
        gates = gates.T[here]

        def one(e, _):
            turn = lax.div(e, own)
            slot = jnp.where(turn == 0, base[0], jnp.where(turn == 1, base[1], jnp.where(turn == 2, base[2], base[3]))) + lax.rem(e, own)
            lane = lax.broadcasted_iota(jnp.int32, gates.shape, 1)
            g = jnp.sum(jnp.where(lane == slot, gates, 0.0), axis=1, keepdims=True)
            u = ubuf[s, here]
            f1 = jnp.dot(u, w1[slot], preferred_element_type=jnp.float32)
            f3 = jnp.dot(u, w3[slot], preferred_element_type=jnp.float32)
            a = (f1 * jax.nn.sigmoid(f1) * f3).astype(jnp.bfloat16)
            for j in range(0, dim, 512):
                o = jnp.dot(a, w2[slot, :, j:j + 512], preferred_element_type=jnp.float32).astype(jnp.bfloat16).astype(jnp.float32)
                part[s, here, j:j + 512] += jnp.where(g != 0.0, g * o, 0.0)
            return 0

        lax.fori_loop(first, first + count, one, 0)

    def gates_of(s):
        if s == 0:
            return g_own[lax.rem(pos, classes)]
        lane = lax.broadcasted_iota(jnp.int32, gbuf.shape[2:], 1)
        return jnp.where(lax.rem(lax.div(lane, ru), 2) == 0, gbuf[0, s - 1], gbuf[1, s - 1])

    def forward(s):
        for p in range(pieces_u):
            for d in range(2):
                u_copy(d, s - 1, p).wait_recv()
                if s < hops:
                    u_copy(d, s, p).start()

    for t in range(3):
        load(t).wait()
    experts(0, gates_of(0), 0, own)
    for s in range(1, hops + 1):
        for d in range(2):
            g_copy(d, s).start()
    for t in range(3):
        hand(0, t).wait()
    share_out(1, 0)
    forward(1)
    experts(0, gates_of(0), own, own)
    share_out(1, 1)
    for s in range(1, hops + 1):
        for d in range(2):
            g_copy(d, s).wait()
    experts(1, gates_of(1), 0, own)
    share_out(2, 0)
    forward(2)
    experts(1, gates_of(1), own, own)
    share_out(2, 1)
    collect(0)
    experts(2, gates_of(2), 0, 2 * own)
    for s in range(3, hops + 1):
        forward(s)
    collect(1)
    experts(hops, gates_of(hops), 0, 2 * own)
    collect(2)
    for p in range(pieces_u):
        experts(hops, gates_of(hops), 2 * own, own, p * 2 * ru, 2 * ru)
        if p == 0:
            for t in range(3):
                hand(1, t).wait_recv()
        experts(hops, gates_of(hops), 3 * own, own, p * 2 * ru, 2 * ru)
        for q in range(p * per, (p + 1) * per):
            for d in range(2):
                a_copy(d, hops, q).start()

    for s in range(hops - 1, -1, -1):
        experts(s, gates_of(s), 2 * own, 2 * own)
        for p in range(pieces_a):
            for d in range(2):
                rows = a_rows(d, p)
                a_copy(d, s + 1, p).wait_recv()
                if s > 0:
                    part[s, rows] += acc[s, rows]
                    a_copy(d, s, p).start()
                else:
                    y_ref[rows] = (y_ref[rows].astype(jnp.float32) + (part[s, rows] + acc[s, rows])).astype(y_ref.dtype)


    def drain_ring(s, _):
        for m in range(mats):
            for d in range(2):
                across(d, s, m).wait_send()

                @pl.when(s < n - 1)
                def _():
                    ring(d, s, m).wait_send()
        return 0

    lax.fori_loop(0, n, drain_ring, 0)

    def drain_groups(j, _):
        for t in range(3):
            for d in range(2):
                spread(t, d, j).wait_send()
        return 0

    lax.fori_loop(1, groups, drain_groups, 0)
    for t in range(3):
        hand(1, t).wait_send()
        for d in range(2):
            fetch(t, d).wait_send()
    for s in range(hops):
        for d in range(2):
            for p in range(pieces_u):
                u_copy(d, s, p).wait_send()
            for p in range(pieces_a):
                a_copy(d, s + 1, p).wait_send()


def layer(x, w_query, w_key, w_value, w_out, w_router_t, ids_t, w_one, w_three, w_two, n, groups, head_dim):
    tok, dim = x.shape
    own, _, ff = w_one.shape
    classes = n // 2
    hops, total = classes - 1, 4 * own
    pieces_u, pieces_a = 2, 4
    dma = pltpu.SemaphoreType.DMA
    any_spec = pl.BlockSpec(memory_space=pl.ANY)
    vmem = pl.BlockSpec(memory_space=pltpu.VMEM)
    bf16, f32 = jnp.bfloat16, jnp.float32
    return pl.pallas_call(
        functools.partial(layer_kernel, n, groups, head_dim, pieces_u=pieces_u, pieces_a=pieces_a),
        out_shape=jax.ShapeDtypeStruct((tok, dim), bf16),
        in_specs=[vmem, any_spec, any_spec, any_spec, any_spec, vmem, vmem, any_spec, any_spec, any_spec],
        out_specs=vmem,
        scratch_shapes=[
            pltpu.VMEM((4, dim, dim), bf16),
            pltpu.VMEM((tok, dim), bf16),
            pltpu.VMEM((3, tok, dim), bf16),
            pltpu.VMEM((hops + 1, tok, dim), bf16),
            pltpu.VMEM((classes, total, tok), f32),
            pltpu.VMEM((2, hops, total, tok), f32),
            pltpu.VMEM((hops + 1, tok, dim), f32),
            pltpu.VMEM((hops, tok, dim), f32),
            pltpu.VMEM((total, dim, ff), bf16),
            pltpu.VMEM((total, dim, ff), bf16),
            pltpu.VMEM((total, ff, dim), bf16),
            dma((2, n, 4)), dma((2, n, 4)), dma((2, n, 4)), dma((2, n, 4)), dma((4,)), dma((3,)),
            dma((3, 2)), dma((3, 2)), dma((3, 2, groups - 1)), dma((3, 2, groups - 1)), dma((2, 3)), dma((2, 3)),
            dma((2, hops, pieces_u)), dma((2, hops, pieces_u)),
            dma((2, hops, pieces_a)), dma((2, hops, pieces_a)),
            dma((2, hops)), dma((2, hops)),
        ],
        compiler_params=pltpu.CompilerParams(collective_id=1, has_side_effects=True, vmem_limit_bytes=67_000_000),
        name='layer_ring',
    )(x, w_query, w_key, w_value, w_out, w_router_t, ids_t, w_one, w_three, w_two)


def solution(mesh):
    tok_spec = P(('dp', 'ep'))
    row_spec = P('ep')
    n = mesh.shape['ep'] // 2
    groups = mesh.shape['dp']

    def local_layer(tokens, w_query, w_key, w_value, w_out, w_router, w_one, w_three, w_two, expert_ids):
        tok, dim = tokens.shape[0] * tokens.shape[1], tokens.shape[2]
        flat = [w.reshape(w.shape[0], -1) for w in (w_query, w_key, w_value)]
        ids_t = expert_ids.reshape(tok, -1).T
        out = layer(tokens.reshape(tok, dim), *flat, w_out, w_router.T, ids_t, w_one, w_three, w_two, n, groups, w_query.shape[2])
        return out.reshape(tokens.shape)

    return jax.shard_map(local_layer, mesh=mesh, in_specs=(tok_spec, row_spec, row_spec, row_spec, row_spec, P(), row_spec, row_spec, row_spec, tok_spec), out_specs=tok_spec, check_vma=False)
```

```python
import functools

import jax
import jax.numpy as jnp
from jax import lax
from jax.experimental import pallas as pl
from jax.experimental.pallas import tpu as pltpu
from jax.sharding import PartitionSpec as P

EPS = 1e-6
MESH = pl.DeviceIdType.MESH


def rms_norm(vals):
    wide = vals.astype(jnp.float32)
    return wide * lax.rsqrt(jnp.mean(wide * wide, axis=-1, keepdims=True) + EPS)


def attend_pair(q_ref, k_ref, v_ref, c_ref, i, scale):
    seq, lanes = q_ref.shape[0], 128
    cols = pl.ds(pl.multiple_of(i * lanes, lanes), lanes)
    step = seq // 2
    lane = lax.broadcasted_iota(jnp.int32, (1, lanes), 1)
    keep = [jnp.where(lane < lanes // 2, 1.0, 0.0).astype(jnp.bfloat16), jnp.where(lane < lanes // 2, 0.0, 1.0).astype(jnp.bfloat16)]
    for b in range(2):
        rows, keys = slice(b * step, (b + 1) * step), (b + 1) * step
        q, k, v = q_ref[rows, cols], k_ref[:keys, cols], v_ref[:keys, cols]
        causal = (lax.broadcasted_iota(jnp.int32, (step, keys), 0) + b * step) >= lax.broadcasted_iota(jnp.int32, (step, keys), 1)
        context = None
        for side in range(2):
            s = lax.dot_general(q * keep[side], k, (((1,), (1,)), ((), ())), preferred_element_type=jnp.float32) * scale
            s = jnp.where(causal, s, -jnp.inf)
            e = jnp.exp(s - jnp.max(s, axis=-1, keepdims=True))
            p = (e * (1.0 / jnp.sum(e, axis=-1, keepdims=True))).astype(jnp.bfloat16)
            c = jnp.dot(p, v * keep[side], preferred_element_type=jnp.float32)
            context = c if context is None else context + c
        c_ref[rows, cols] = context.astype(jnp.bfloat16)


def layer_kernel(n, groups, head_dim, x_ref, wq_hbm, wk_hbm, wv_hbm, wo_hbm, wr_ref, ids_ref, e1_hbm, e3_hbm, e2_hbm, y_ref,
                 wbuf, nbuf, qkv, ubuf, g_own, gbuf, part, acc, w1, w3, w2,
                 b_send, b_recv, c_send, c_recv, d_send, d_recv, loc, w_loc, z_send, z_recv, s_send, s_recv, w_send, w_recv,
                 u_send, u_recv, a_send, a_recv, g_send, g_recv, *, pieces_u, pieces_a):
    me, group = lax.axis_index('ep'), lax.axis_index('dp')
    pos, core = lax.div(me, 2), lax.rem(me, 2)
    share = wq_hbm.shape[0]
    mats = wbuf.shape[0]
    tok, dim = x_ref.shape
    own, classes = e1_hbm.shape[0], g_own.shape[0]
    hops = classes - 1
    ru = tok // (2 * pieces_u)
    per = pieces_a // pieces_u
    ra = ru // per

    def peer(z):
        return {'ep': lax.rem(z, n) * 2 + core}

    def other(j):
        return {'dp': lax.rem(group + j, groups)}

    sibling = {'ep': pos * 2 + (1 - core)}

    def remote(src, dst, send, recv, device):
        return pltpu.make_async_remote_copy(src_ref=src, dst_ref=dst, send_sem=send, recv_sem=recv, device_id=device, device_id_type=MESH)

    barrier = pltpu.get_barrier_semaphore()

    def greet_ring(k, _):
        pl.semaphore_signal(barrier, inc=1, device_id=peer(pos + k), device_id_type=MESH)
        return 0

    def greet_groups(j, _):
        pl.semaphore_signal(barrier, inc=1, device_id=other(j), device_id_type=MESH)
        return 0

    lax.fori_loop(1, n, greet_ring, 0)
    lax.fori_loop(1, groups, greet_groups, 0)
    pl.semaphore_signal(barrier, inc=1, device_id=sibling, device_id_type=MESH)


    parts, whole = max(1, groups // mats), max(1, mats // groups)
    first_mat, first_row = lax.div(group * mats, groups), lax.rem(group, parts) * (share // parts)
    order = sorted(range(n), key=lambda k: min(k, n - k))

    def piece(k):
        return wbuf.at[pl.ds(first_mat, whole), lax.rem(pos + n - k, n), core, pl.ds(pl.multiple_of(first_row, share // parts), share // parts)]

    def along(k):
        return remote(piece(0), piece(0), b_send.at[k], b_recv.at[k], peer(pos + k))

    def outward(k, j):
        return remote(piece(k), piece(k), c_send.at[k, j - 1], c_recv.at[k, j - 1], other(j))

    def across(k):
        block = wbuf.at[:, lax.rem(pos + n - k, n), core]
        return remote(block, block, d_send.at[k], d_recv.at[k], sibling)

    def each_group(do):
        def step(j, _):
            do(j)
            return 0

        lax.fori_loop(1, groups, step, 0)


    near, away = lax.div(pos, classes) * 2 * own, (1 - lax.div(pos, classes)) * 2 * own
    base = [near + core * own, near + (1 - core) * own, away + core * own, away + (1 - core) * own]
    experts_of = ((e1_hbm, w1), (e3_hbm, w3), (e2_hbm, w2))

    def rows_of(t, d):
        size = experts_of[t][0].shape[1] // (2 * groups)
        return pl.ds(pl.multiple_of((group * 2 + d) * size, size), size)

    def load(t):
        return pltpu.make_async_copy(experts_of[t][0], experts_of[t][1].at[pl.ds(base[0], own)], w_loc.at[t])

    def hand(r, t):
        kept = experts_of[t][1].at[pl.ds(base[2 * r], own)]
        return remote(experts_of[t][0] if r == 0 else kept, kept, w_send.at[r, t], w_recv.at[r, t], sibling)

    def fetch(t, d):
        rows = rows_of(t, d)
        return remote(experts_of[t][0].at[:, rows], experts_of[t][1].at[pl.ds(base[0], own), rows], z_send.at[t, d], z_recv.at[t, d], peer(pos + n // 2))

    def spread(t, d, j):
        piece = experts_of[t][1].at[pl.ds(base[2], own), rows_of(t, d)]
        return remote(piece, piece, s_send.at[t, d, j - 1], s_recv.at[t, d, j - 1], other(j))

    def share_out(t, d):
        fetch(t, d).wait_recv()

        def send(j, _):
            spread(t, d, j).start()
            return 0

        lax.fori_loop(1, groups, send, 0)

    def collect(t):
        def take(j, _):
            for d in range(2):
                spread(t, d, j).wait_recv()
            return 0

        lax.fori_loop(1, groups, take, 0)
        hand(1, t).start()

    shards = []
    for m, src in enumerate((wq_hbm, wk_hbm, wv_hbm, wo_hbm)):
        shards.append(pltpu.make_async_copy(src, wbuf.at[m, pos, core], loc.at[m]))
        shards[-1].start()
    for t in range(3):
        load(t).start()
    pl.semaphore_wait(barrier, n + groups - 1)
    for m in range(mats):
        shards[m].wait()
    for k in order[1:]:
        along(k).start()
    for t in range(3):
        for d in range(2):
            fetch(t, d).start()
    for t in range(3):
        hand(0, t).start()
    nbuf[...] = rms_norm(x_ref[...]).astype(jnp.bfloat16)
    for s in range(hops + 1):
        part[s] = jnp.zeros(part.shape[1:], jnp.float32)

    for k in order[1:]:
        along(k).wait_recv()
        each_group(lambda j: outward(k, j).start())
    across(0).start()
    for k in order[1:]:
        each_group(lambda j: outward(k, j).wait_recv())
        across(k).start()
    share_out(0, 0)
    share_out(0, 1)
    for k in order:
        across(k).wait_recv()
    width = dim // 2

    def project(j, _):
        m, c = lax.div(j, 2), lax.rem(j, 2)
        cols = pl.ds(pl.multiple_of(c * width, width), width)
        qkv[m, :, cols] = jnp.dot(nbuf[...], wbuf[m, :, :, :, cols].reshape(dim, width), preferred_element_type=jnp.float32).astype(jnp.bfloat16)
        return 0

    lax.fori_loop(0, 6, project, 0)
    pairs = dim // 128

    def heads(i, _):
        attend_pair(qkv.at[0], qkv.at[1], qkv.at[2], nbuf, i, head_dim ** -0.5)

        @pl.when(i == pairs // 4)
        def _():
            share_out(1, 0)

        @pl.when(i == 3 * pairs // 4)
        def _():
            share_out(1, 1)
        return 0

    lax.fori_loop(0, pairs, heads, 0)
    for j in range(2):
        cols = slice(j * width, (j + 1) * width)
        mixed = jnp.dot(nbuf[...], wbuf[3, :, :, :, cols].reshape(dim, width), preferred_element_type=jnp.float32)
        y_ref[:, cols] = (x_ref[:, cols].astype(jnp.float32) + mixed).astype(jnp.bfloat16)
    z = rms_norm(y_ref[...])
    ubuf[0] = z.astype(jnp.bfloat16)
    logits = lax.dot_general(wr_ref[...], z, (((1,), (1,)), ((), ())), precision=lax.Precision.HIGHEST, preferred_element_type=jnp.float32)
    expert = lax.broadcasted_iota(jnp.int32, logits.shape, 0)
    match = expert == ids_ref[0:1, :]
    for j in range(1, ids_ref.shape[0]):
        match = match | (expert == ids_ref[j:j + 1, :])
    logits = jnp.where(match, logits, -jnp.inf)
    e = jnp.where(match, jnp.exp(logits - jnp.max(logits, axis=0, keepdims=True)), 0.0)
    gates = e / jnp.sum(e, axis=0, keepdims=True)
    layer = gates.shape[0] // n
    for c in range(classes):
        g_own[c] = jnp.concatenate([gates[(c + r * classes) * layer:(c + r * classes + 1) * layer] for r in range(n // classes)], axis=0)


    def u_copy(d, s, p):
        rows = pl.ds((2 * p + d) * ru, ru)
        return remote(ubuf.at[s, rows], ubuf.at[s + 1, rows], u_send.at[d, s, p], u_recv.at[d, s, p], peer(pos + (1 if d == 0 else n - 1)))

    def a_rows(d, p):
        return pl.ds((2 * (p // per) + d) * ru + (p % per) * ra, ra)

    def a_copy(d, s, p):
        rows = a_rows(d, p)
        return remote(part.at[s, rows], acc.at[s - 1, rows], a_send.at[d, s - 1, p], a_recv.at[d, s - 1, p], peer(pos + (n - 1 if d == 0 else 1)))

    def g_copy(d, s):
        target = pos + (s if d == 0 else n - s)
        return remote(g_own.at[lax.rem(target, classes)], gbuf.at[d, s - 1], g_send.at[d, s - 1], g_recv.at[d, s - 1], peer(target))

    for p in range(pieces_u):
        for d in range(2):
            u_copy(d, 0, p).start()

    def experts(s, gates, first, count, start=0, rows=tok):
        here = slice(start, start + rows)
        gates = gates.T[here]

        def one(e, _):
            turn = lax.div(e, own)
            slot = jnp.where(turn == 0, base[0], jnp.where(turn == 1, base[1], jnp.where(turn == 2, base[2], base[3]))) + lax.rem(e, own)
            lane = lax.broadcasted_iota(jnp.int32, gates.shape, 1)
            g = jnp.sum(jnp.where(lane == slot, gates, 0.0), axis=1, keepdims=True)
            u = ubuf[s, here]
            f1 = jnp.dot(u, w1[slot], preferred_element_type=jnp.float32)
            f3 = jnp.dot(u, w3[slot], preferred_element_type=jnp.float32)
            a = (f1 * jax.nn.sigmoid(f1) * f3).astype(jnp.bfloat16)
            for j in range(0, dim, 512):
                o = jnp.dot(a, w2[slot, :, j:j + 512], preferred_element_type=jnp.float32).astype(jnp.bfloat16).astype(jnp.float32)
                part[s, here, j:j + 512] += jnp.where(g != 0.0, g * o, 0.0)
            return 0

        lax.fori_loop(first, first + count, one, 0)

    def gates_of(s):
        if s == 0:
            return g_own[lax.rem(pos, classes)]
        lane = lax.broadcasted_iota(jnp.int32, gbuf.shape[2:], 1)
        return jnp.where(lax.rem(lax.div(lane, ru), 2) == 0, gbuf[0, s - 1], gbuf[1, s - 1])

    def forward(s, first=0, last=pieces_u):
        for p in range(first, last):
            for d in range(2):
                u_copy(d, s - 1, p).wait_recv()
                if s < hops:
                    u_copy(d, s, p).start()

    for t in range(3):
        load(t).wait()
    for s in range(1, hops + 1):
        for d in range(2):
            g_copy(d, s).start()
    experts(0, gates_of(0), 0, own)
    share_out(2, 0)
    for t in range(3):
        hand(0, t).wait()
    collect(0)
    experts(0, gates_of(0), own, own)
    forward(1)
    share_out(2, 1)
    for s in range(1, hops + 1):
        for d in range(2):
            g_copy(d, s).wait()
    experts(1, gates_of(1), 0, 2 * own)
    forward(2)
    collect(1)
    experts(2, gates_of(2), 0, 2 * own)
    for s in range(3, hops):
        forward(s)
    collect(2)
    for t in range(3):
        hand(1, t).wait_recv()
    for p in range(pieces_u):
        forward(hops, p, p + 1)
        experts(hops, gates_of(hops), 0, 4 * own, p * 2 * ru, 2 * ru)
        for q in range(p * per, (p + 1) * per):
            for d in range(2):
                a_copy(d, hops, q).start()

    for s in range(hops - 1, -1, -1):
        experts(s, gates_of(s), 2 * own, 2 * own)
        for p in range(pieces_a):
            for d in range(2):
                rows = a_rows(d, p)
                a_copy(d, s + 1, p).wait_recv()
                if s > 0:
                    part[s, rows] += acc[s, rows]
                    a_copy(d, s, p).start()
                else:
                    y_ref[rows] = (y_ref[rows].astype(jnp.float32) + (part[s, rows] + acc[s, rows])).astype(y_ref.dtype)


    for k in order:
        across(k).wait_send()
        if k:
            along(k).wait_send()
            each_group(lambda j: outward(k, j).wait_send())

    def drain_groups(j, _):
        for t in range(3):
            for d in range(2):
                spread(t, d, j).wait_send()
        return 0

    lax.fori_loop(1, groups, drain_groups, 0)
    for t in range(3):
        hand(1, t).wait_send()
        for d in range(2):
            fetch(t, d).wait_send()
    for s in range(hops):
        for d in range(2):
            for p in range(pieces_u):
                u_copy(d, s, p).wait_send()
            for p in range(pieces_a):
                a_copy(d, s + 1, p).wait_send()


def layer(x, w_query, w_key, w_value, w_out, w_router_t, ids_t, w_one, w_three, w_two, n, groups, head_dim):
    tok, dim = x.shape
    own, _, ff = w_one.shape
    classes = n // 2
    hops, total = classes - 1, 4 * own
    pieces_u, pieces_a = 2, 4
    dma = pltpu.SemaphoreType.DMA
    any_spec = pl.BlockSpec(memory_space=pl.ANY)
    vmem = pl.BlockSpec(memory_space=pltpu.VMEM)
    bf16, f32 = jnp.bfloat16, jnp.float32
    return pl.pallas_call(
        functools.partial(layer_kernel, n, groups, head_dim, pieces_u=pieces_u, pieces_a=pieces_a),
        out_shape=jax.ShapeDtypeStruct((tok, dim), bf16),
        in_specs=[vmem, any_spec, any_spec, any_spec, any_spec, vmem, vmem, any_spec, any_spec, any_spec],
        out_specs=vmem,
        scratch_shapes=[
            pltpu.VMEM((4, n, 2, w_query.shape[0], dim), bf16),
            pltpu.VMEM((tok, dim), bf16),
            pltpu.VMEM((3, tok, dim), bf16),
            pltpu.VMEM((hops + 1, tok, dim), bf16),
            pltpu.VMEM((classes, total, tok), f32),
            pltpu.VMEM((2, hops, total, tok), f32),
            pltpu.VMEM((hops + 1, tok, dim), f32),
            pltpu.VMEM((hops, tok, dim), f32),
            pltpu.VMEM((total, dim, ff), bf16),
            pltpu.VMEM((total, dim, ff), bf16),
            pltpu.VMEM((total, ff, dim), bf16),
            dma((n,)), dma((n,)), dma((n, groups - 1)), dma((n, groups - 1)), dma((n,)), dma((n,)), dma((4,)), dma((3,)),
            dma((3, 2)), dma((3, 2)), dma((3, 2, groups - 1)), dma((3, 2, groups - 1)), dma((2, 3)), dma((2, 3)),
            dma((2, hops, pieces_u)), dma((2, hops, pieces_u)),
            dma((2, hops, pieces_a)), dma((2, hops, pieces_a)),
            dma((2, hops)), dma((2, hops)),
        ],
        compiler_params=pltpu.CompilerParams(collective_id=1, has_side_effects=True, vmem_limit_bytes=67_000_000),
        name='layer_ring',
    )(x, w_query, w_key, w_value, w_out, w_router_t, ids_t, w_one, w_three, w_two)


def solution(mesh):
    tok_spec = P(('dp', 'ep'))
    row_spec = P('ep')
    n = mesh.shape['ep'] // 2
    groups = mesh.shape['dp']

    def local_layer(tokens, w_query, w_key, w_value, w_out, w_router, w_one, w_three, w_two, expert_ids):
        tok, dim = tokens.shape[0] * tokens.shape[1], tokens.shape[2]
        flat = [w.reshape(w.shape[0], -1) for w in (w_query, w_key, w_value)]
        ids_t = expert_ids.reshape(tok, -1).T
        out = layer(tokens.reshape(tok, dim), *flat, w_out, w_router.T, ids_t, w_one, w_three, w_two, n, groups, w_query.shape[2])
        return out.reshape(tokens.shape)

    return jax.shard_map(local_layer, mesh=mesh, in_specs=(tok_spec, row_spec, row_spec, row_spec, row_spec, P(), row_spec, row_spec, row_spec, tok_spec), out_specs=tok_spec, check_vma=False)
```

```python
import functools
import math

import jax
import jax.numpy as jnp
from jax import lax
from jax.experimental import pallas as pl
from jax.experimental.pallas import tpu as pltpu
from jax.sharding import PartitionSpec as P

EPS = 1e-6
MESH = pl.DeviceIdType.MESH


def rms_norm(vals):
    wide = vals.astype(jnp.float32)
    return wide * lax.rsqrt(jnp.mean(wide * wide, axis=-1, keepdims=True) + EPS)


def attend_pair(q_ref, k_ref, v_ref, c_ref, i, scale):
    seq, lanes = q_ref.shape[0], 128
    cols = pl.ds(pl.multiple_of(i * lanes, lanes), lanes)
    step = seq // 2
    lane = lax.broadcasted_iota(jnp.int32, (1, lanes), 1)
    keep = [jnp.where(lane < lanes // 2, 1.0, 0.0).astype(jnp.bfloat16), jnp.where(lane < lanes // 2, 0.0, 1.0).astype(jnp.bfloat16)]
    for b in range(2):
        rows, keys = slice(b * step, (b + 1) * step), (b + 1) * step
        q, k, v = q_ref[rows, cols], k_ref[:keys, cols], v_ref[:keys, cols]
        causal = (lax.broadcasted_iota(jnp.int32, (step, keys), 0) + b * step) >= lax.broadcasted_iota(jnp.int32, (step, keys), 1)
        context = None
        for side in range(2):
            s = lax.dot_general(q * keep[side], k, (((1,), (1,)), ((), ())), preferred_element_type=jnp.float32) * scale
            s = jnp.where(causal, s, -jnp.inf)
            e = jnp.exp(s - jnp.max(s, axis=-1, keepdims=True))
            p = (e * (1.0 / jnp.sum(e, axis=-1, keepdims=True))).astype(jnp.bfloat16)
            c = jnp.dot(p, v * keep[side], preferred_element_type=jnp.float32)
            context = c if context is None else context + c
        c_ref[rows, cols] = context.astype(jnp.bfloat16)


def layer_kernel(n, groups, head_dim, x_ref, wqkv_hbm, wo_hbm, wr_ref, ids_ref, e1_hbm, e3_hbm, e2_hbm, y_ref,
                 wbuf, nbuf, qkv, ubuf, g_own, gbuf, part, acc, w1, w3, w2,
                 b_send, b_recv, c_send, c_recv, c2_send, c2_recv, d_send, d_recv, loc, w_loc, z_send, z_recv, s_send, s_recv, s2_send, s2_recv, w_send, w_recv,
                 u_send, u_recv, a_send, a_recv, g_send, g_recv, *, pieces_u, pieces_a):
    me, group = lax.axis_index('ep'), lax.axis_index('dp')
    pos, core = lax.div(me, 2), lax.rem(me, 2)
    share = wo_hbm.shape[0]
    mats = wbuf.shape[0]
    tok, dim = x_ref.shape
    own, classes = e1_hbm.shape[0], g_own.shape[0]
    hops = classes - 1
    ru = tok // (2 * pieces_u)
    per = pieces_a // pieces_u
    ra = ru // per

    def peer(z):
        return {'ep': lax.rem(z, n) * 2 + core}


    low = math.isqrt(groups) if math.isqrt(groups) ** 2 == groups else groups
    sides = (low, groups // low)
    spots = (lax.rem(group, low), lax.div(group, low))

    def member(f, i, j):
        at = [0, 0]
        at[f] = lax.rem(spots[f] + i + sides[f], sides[f])
        at[1 - f] = lax.rem(spots[1 - f] + j + sides[1 - f], sides[1 - f])
        return at[1] * low + at[0]

    def swap_first(f, piece, sems, i):
        return remote(piece(group), piece(group), sems[0].at[i - 1], sems[1].at[i - 1], {'dp': member(f, i, 0)})

    def swap_then(f, piece, sems, i, j):
        ref, at = piece(member(f, -i, 0)), i * (sides[1 - f] - 1) + j - 1
        return remote(ref, ref, sems[2].at[at], sems[3].at[at], {'dp': member(f, 0, j)})

    def firsts(f):
        return range(1, sides[f])

    def thens(f):
        return range(1, sides[1 - f])

    def swap_start(f, piece, sems):
        for i in firsts(f):
            swap_first(f, piece, sems, i).start()
        for j in thens(f):
            swap_then(f, piece, sems, 0, j).start()

    def swap_relay(f, piece, sems):
        for i in firsts(f):
            swap_first(f, piece, sems, i).wait_recv()
            for j in thens(f):
                swap_then(f, piece, sems, i, j).start()

    def swap_take(f, piece, sems):
        for i in range(sides[f]):
            for j in thens(f):
                swap_then(f, piece, sems, i, j).wait_recv()

    def swap_drain(f, piece, sems):
        for i in firsts(f):
            swap_first(f, piece, sems, i).wait_send()
        for i in range(sides[f]):
            for j in thens(f):
                swap_then(f, piece, sems, i, j).wait_send()

    sibling = {'ep': pos * 2 + (1 - core)}

    def remote(src, dst, send, recv, device):
        return pltpu.make_async_remote_copy(src_ref=src, dst_ref=dst, send_sem=send, recv_sem=recv, device_id=device, device_id_type=MESH)

    barrier = pltpu.get_barrier_semaphore()

    def greet_ring(k, _):
        pl.semaphore_signal(barrier, inc=1, device_id=peer(pos + k), device_id_type=MESH)
        return 0

    def greet_groups(j, _):
        pl.semaphore_signal(barrier, inc=1, device_id={'dp': lax.rem(group + j, groups)}, device_id_type=MESH)
        return 0

    lax.fori_loop(1, n, greet_ring, 0)
    lax.fori_loop(1, groups, greet_groups, 0)
    pl.semaphore_signal(barrier, inc=1, device_id=sibling, device_id_type=MESH)


    parts, whole = max(1, groups // mats), max(1, mats // groups)
    order = sorted(range(n), key=lambda k: min(k, n - k))

    def shard_piece(k, g):
        row = pl.multiple_of(lax.rem(g, parts) * (share // parts), share // parts)
        return wbuf.at[pl.ds(lax.div(g * mats, groups), whole), lax.rem(pos + n - k, n), core, pl.ds(row, share // parts)]

    def along(k):
        return remote(shard_piece(0, group), shard_piece(0, group), b_send.at[k], b_recv.at[k], peer(pos + k))

    def outward(k):
        return k % 2, functools.partial(shard_piece, k), [r.at[k] for r in (c_send, c_recv, c2_send, c2_recv)]

    def across(k):
        block = wbuf.at[:, lax.rem(pos + n - k, n), core]
        return remote(block, block, d_send.at[k], d_recv.at[k], sibling)


    near, away = lax.div(pos, classes) * 2 * own, (1 - lax.div(pos, classes)) * 2 * own
    base = [near + core * own, near + (1 - core) * own, away + core * own, away + (1 - core) * own]
    experts_of = ((e1_hbm, w1), (e3_hbm, w3), (e2_hbm, w2))

    def rows_of(t, d, g):
        size = experts_of[t][0].shape[1] // (2 * groups)
        return pl.ds(pl.multiple_of((g * 2 + d) * size, size), size)

    def load(t):
        return pltpu.make_async_copy(experts_of[t][0], experts_of[t][1].at[pl.ds(base[0], own)], w_loc.at[t])

    def hand(r, t):
        kept = experts_of[t][1].at[pl.ds(base[2 * r], own)]
        return remote(experts_of[t][0] if r == 0 else kept, kept, w_send.at[r, t], w_recv.at[r, t], sibling)

    def fetch(t, d):
        rows = rows_of(t, d, group)
        return remote(experts_of[t][0].at[:, rows], experts_of[t][1].at[pl.ds(base[0], own), rows], z_send.at[t, d], z_recv.at[t, d], peer(pos + n // 2))

    def spread(t, d):
        def expert_piece(g):
            return experts_of[t][1].at[pl.ds(base[2], own), rows_of(t, d, g)]

        return d, expert_piece, [r.at[t, d] for r in (s_send, s_recv, s2_send, s2_recv)]

    def share_out(t, d):
        fetch(t, d).wait_recv()
        swap_start(*spread(t, d))

    def share_on(t, d):
        swap_relay(*spread(t, d))

    def collect(t):
        for d in range(2):
            swap_take(*spread(t, d))
        hand(1, t).start()

    shards = []
    for m, src in enumerate((wqkv_hbm.at[0], wqkv_hbm.at[1], wqkv_hbm.at[2], wo_hbm)):
        shards.append(pltpu.make_async_copy(src, wbuf.at[m, pos, core], loc.at[m]))
        shards[-1].start()
    for t in range(3):
        load(t).start()
    pl.semaphore_wait(barrier, n + groups - 1)
    for m in range(mats):
        shards[m].wait()
    for k in order[1:]:
        along(k).start()
    for t in range(3):
        hand(0, t).start()
    nbuf[...] = rms_norm(x_ref[...]).astype(jnp.bfloat16)
    for s in range(hops + 1):
        part[s] = jnp.zeros(part.shape[1:], jnp.float32)

    across(0).start()
    for i in range(n + 1):
        if i + 1 < n:
            along(order[i + 1]).wait_recv()
            swap_start(*outward(order[i + 1]))
        if i == n // 2 - 1:
            for t in range(3):
                for d in range(2):
                    fetch(t, d).start()
        if i > 1:
            swap_relay(*outward(order[i - 1]))
    share_out(0, 0)
    for k in order[1:]:
        swap_take(*outward(k))
        across(k).start()
    for k in order:
        across(k).wait_recv()
    width = dim // 2

    def project(j, _):
        m, c = lax.div(j, 2), lax.rem(j, 2)
        cols = pl.ds(pl.multiple_of(c * width, width), width)
        qkv[m, :, cols] = jnp.dot(nbuf[...], wbuf[m, :, :, :, cols].reshape(dim, width), preferred_element_type=jnp.float32).astype(jnp.bfloat16)
        return 0

    lax.fori_loop(0, 6, project, 0)
    share_out(0, 1)
    share_on(0, 0)
    pairs = dim // 128

    def heads(i, _):
        attend_pair(qkv.at[0], qkv.at[1], qkv.at[2], nbuf, i, head_dim ** -0.5)

        @pl.when(i == pairs // 4)
        def _():
            share_on(0, 1)

        @pl.when(i == 5 * pairs // 8)
        def _():
            share_out(1, 0)
        return 0

    lax.fori_loop(0, pairs, heads, 0)
    share_on(1, 0)
    for j in range(2):
        cols = slice(j * width, (j + 1) * width)
        mixed = jnp.dot(nbuf[...], wbuf[3, :, :, :, cols].reshape(dim, width), preferred_element_type=jnp.float32)
        y_ref[:, cols] = (x_ref[:, cols].astype(jnp.float32) + mixed).astype(jnp.bfloat16)
    share_out(1, 1)
    z = rms_norm(y_ref[...])
    ubuf[0] = z.astype(jnp.bfloat16)
    logits = lax.dot_general(wr_ref[...], z, (((1,), (1,)), ((), ())), precision=lax.Precision.HIGHEST, preferred_element_type=jnp.float32)
    expert = lax.broadcasted_iota(jnp.int32, logits.shape, 0)
    match = expert == ids_ref[0:1, :]
    for j in range(1, ids_ref.shape[0]):
        match = match | (expert == ids_ref[j:j + 1, :])
    logits = jnp.where(match, logits, -jnp.inf)
    e = jnp.where(match, jnp.exp(logits - jnp.max(logits, axis=0, keepdims=True)), 0.0)
    gates = e / jnp.sum(e, axis=0, keepdims=True)
    layer = gates.shape[0] // n
    for c in range(classes):
        g_own[c] = jnp.concatenate([gates[(c + r * classes) * layer:(c + r * classes + 1) * layer] for r in range(n // classes)], axis=0)


    def u_copy(d, s, p):
        rows = pl.ds((2 * p + d) * ru, ru)
        return remote(ubuf.at[s, rows], ubuf.at[s + 1, rows], u_send.at[d, s, p], u_recv.at[d, s, p], peer(pos + (1 if d == 0 else n - 1)))

    def a_rows(d, p):
        return pl.ds((2 * (p // per) + d) * ru + (p % per) * ra, ra)

    def a_copy(d, s, p):
        rows = a_rows(d, p)
        return remote(part.at[s, rows], acc.at[s - 1, rows], a_send.at[d, s - 1, p], a_recv.at[d, s - 1, p], peer(pos + (n - 1 if d == 0 else 1)))

    def g_copy(d, s):
        target = pos + (s if d == 0 else n - s)
        return remote(g_own.at[lax.rem(target, classes)], gbuf.at[d, s - 1], g_send.at[d, s - 1], g_recv.at[d, s - 1], peer(target))

    for p in range(pieces_u):
        for d in range(2):
            u_copy(d, 0, p).start()

    def experts(s, gates, first, count, start=0, rows=tok):
        here = slice(start, start + rows)
        gates = gates.T[here]

        def one(e, _):
            turn = lax.div(e, own)
            slot = jnp.where(turn == 0, base[0], jnp.where(turn == 1, base[1], jnp.where(turn == 2, base[2], base[3]))) + lax.rem(e, own)
            lane = lax.broadcasted_iota(jnp.int32, gates.shape, 1)
            g = jnp.sum(jnp.where(lane == slot, gates, 0.0), axis=1, keepdims=True)
            u = ubuf[s, here]
            f1 = jnp.dot(u, w1[slot], preferred_element_type=jnp.float32)
            f3 = jnp.dot(u, w3[slot], preferred_element_type=jnp.float32)
            a = (f1 * jax.nn.sigmoid(f1) * f3).astype(jnp.bfloat16)
            for j in range(0, dim, 512):
                o = jnp.dot(a, w2[slot, :, j:j + 512], preferred_element_type=jnp.float32).astype(jnp.bfloat16).astype(jnp.float32)
                part[s, here, j:j + 512] += jnp.where(g != 0.0, g * o, 0.0)
            return 0

        lax.fori_loop(first, first + count, one, 0)

    def gates_of(s):
        if s == 0:
            return g_own[lax.rem(pos, classes)]
        lane = lax.broadcasted_iota(jnp.int32, gbuf.shape[2:], 1)
        return jnp.where(lax.rem(lax.div(lane, ru), 2) == 0, gbuf[0, s - 1], gbuf[1, s - 1])

    def forward(s, first=0, last=pieces_u):
        for p in range(first, last):
            for d in range(2):
                u_copy(d, s - 1, p).wait_recv()
                if s < hops:
                    u_copy(d, s, p).start()

    for t in range(3):
        load(t).wait()
    for s in range(1, hops + 1):
        for d in range(2):
            g_copy(d, s).start()
    share_on(1, 1)
    share_out(2, 0)
    experts(0, gates_of(0), 0, own)
    for t in range(3):
        hand(0, t).wait()
    collect(0)
    experts(0, gates_of(0), own, own)
    share_on(2, 0)
    share_out(2, 1)
    forward(1)
    for s in range(1, hops + 1):
        for d in range(2):
            g_copy(d, s).wait()
    experts(1, gates_of(1), 0, own)
    share_on(2, 1)
    collect(1)
    experts(1, gates_of(1), own, own)
    forward(2)
    collect(2)
    experts(2, gates_of(2), 0, 2 * own)
    for s in range(3, hops):
        forward(s)
    for t in range(3):
        hand(1, t).wait_recv()
    for p in range(pieces_u):
        forward(hops, p, p + 1)
        experts(hops, gates_of(hops), 0, 4 * own, p * 2 * ru, 2 * ru)
        for q in range(p * per, (p + 1) * per):
            for d in range(2):
                a_copy(d, hops, q).start()

    for s in range(hops - 1, -1, -1):
        experts(s, gates_of(s), 2 * own, 2 * own)
        for p in range(pieces_a):
            for d in range(2):
                rows = a_rows(d, p)
                a_copy(d, s + 1, p).wait_recv()
                if s > 0:
                    part[s, rows] += acc[s, rows]
                    a_copy(d, s, p).start()
                else:
                    y_ref[rows] = (y_ref[rows].astype(jnp.float32) + (part[s, rows] + acc[s, rows])).astype(y_ref.dtype)


    for k in order:
        across(k).wait_send()
        if k:
            along(k).wait_send()
            swap_drain(*outward(k))

    for t in range(3):
        for d in range(2):
            swap_drain(*spread(t, d))
    for t in range(3):
        hand(1, t).wait_send()
        for d in range(2):
            fetch(t, d).wait_send()
    for s in range(hops):
        for d in range(2):
            for p in range(pieces_u):
                u_copy(d, s, p).wait_send()
            for p in range(pieces_a):
                a_copy(d, s + 1, p).wait_send()


def layer(x, w_qkv, w_out, w_router_t, ids_t, w_one, w_three, w_two, n, groups, head_dim):
    tok, dim = x.shape
    own, _, ff = w_one.shape
    classes = n // 2
    hops, total = classes - 1, 4 * own
    pieces_u, pieces_a = 2, 4
    dma = pltpu.SemaphoreType.DMA
    any_spec = pl.BlockSpec(memory_space=pl.ANY)
    vmem = pl.BlockSpec(memory_space=pltpu.VMEM)
    bf16, f32 = jnp.bfloat16, jnp.float32
    return pl.pallas_call(
        functools.partial(layer_kernel, n, groups, head_dim, pieces_u=pieces_u, pieces_a=pieces_a),
        out_shape=jax.ShapeDtypeStruct((tok, dim), bf16),
        in_specs=[vmem, any_spec, any_spec, vmem, vmem, any_spec, any_spec, any_spec],
        out_specs=vmem,
        scratch_shapes=[
            pltpu.VMEM((4, n, 2, w_out.shape[0], dim), bf16),
            pltpu.VMEM((tok, dim), bf16),
            pltpu.VMEM((3, tok, dim), bf16),
            pltpu.VMEM((hops + 1, tok, dim), bf16),
            pltpu.VMEM((classes, total, tok), f32),
            pltpu.VMEM((2, hops, total, tok), f32),
            pltpu.VMEM((hops + 1, tok, dim), f32),
            pltpu.VMEM((hops, tok, dim), f32),
            pltpu.VMEM((total, dim, ff), bf16),
            pltpu.VMEM((total, dim, ff), bf16),
            pltpu.VMEM((total, ff, dim), bf16),
            dma((n,)), dma((n,)), *(dma((n, groups)) for _ in range(4)), dma((n,)), dma((n,)), dma((4,)), dma((3,)),
            dma((3, 2)), dma((3, 2)), *(dma((3, 2, groups)) for _ in range(4)), dma((2, 3)), dma((2, 3)),
            dma((2, hops, pieces_u)), dma((2, hops, pieces_u)),
            dma((2, hops, pieces_a)), dma((2, hops, pieces_a)),
            dma((2, hops)), dma((2, hops)),
        ],
        compiler_params=pltpu.CompilerParams(collective_id=1, has_side_effects=True, vmem_limit_bytes=67_000_000),
        name='layer_ring',
    )(x, w_qkv, w_out, w_router_t, ids_t, w_one, w_three, w_two)


def solution(mesh):
    tok_spec = P(('dp', 'ep'))
    row_spec = P('ep')
    n = mesh.shape['ep'] // 2
    groups = mesh.shape['dp']

    def local_layer(tokens, w_query, w_key, w_value, w_out, w_router, w_one, w_three, w_two, expert_ids):
        tok, dim = tokens.shape[0] * tokens.shape[1], tokens.shape[2]
        flat = jnp.stack([w_query, w_key, w_value]).reshape(3, w_query.shape[0], -1)
        ids_t = expert_ids.reshape(tok, -1).T
        out = layer(tokens.reshape(tok, dim), flat, w_out, w_router.T, ids_t, w_one, w_three, w_two, n, groups, w_query.shape[2])
        return out.reshape(tokens.shape)

    return jax.shard_map(local_layer, mesh=mesh, in_specs=(tok_spec, row_spec, row_spec, row_spec, row_spec, P(), row_spec, row_spec, row_spec, tok_spec), out_specs=tok_spec, check_vma=False)
```

```python
import functools
import math

import jax
import jax.numpy as jnp
from jax import lax
from jax.experimental import pallas as pl
from jax.experimental.pallas import tpu as pltpu
from jax.sharding import PartitionSpec as P

EPS = 1e-6
MESH = pl.DeviceIdType.MESH


def rms_norm(vals):
    wide = vals.astype(jnp.float32)
    return wide * lax.rsqrt(jnp.mean(wide * wide, axis=-1, keepdims=True) + EPS)


def attend_pair(q_ref, k_ref, v_ref, c_ref, i, scale):
    seq, lanes = q_ref.shape[0], 128
    cols = pl.ds(pl.multiple_of(i * lanes, lanes), lanes)
    step = seq // 2
    lane = lax.broadcasted_iota(jnp.int32, (1, lanes), 1)
    keep = [jnp.where(lane < lanes // 2, 1.0, 0.0).astype(jnp.bfloat16), jnp.where(lane < lanes // 2, 0.0, 1.0).astype(jnp.bfloat16)]
    for b in range(2):
        rows, keys = slice(b * step, (b + 1) * step), (b + 1) * step
        q, k, v = q_ref[rows, cols], k_ref[:keys, cols], v_ref[:keys, cols]
        causal = (lax.broadcasted_iota(jnp.int32, (step, keys), 0) + b * step) >= lax.broadcasted_iota(jnp.int32, (step, keys), 1)
        context = None
        for side in range(2):
            s = lax.dot_general(q * keep[side], k, (((1,), (1,)), ((), ())), preferred_element_type=jnp.float32) * scale
            s = jnp.where(causal, s, -jnp.inf)
            e = jnp.exp(s - jnp.max(s, axis=-1, keepdims=True))
            p = (e * (1.0 / jnp.sum(e, axis=-1, keepdims=True))).astype(jnp.bfloat16)
            c = jnp.dot(p, v * keep[side], preferred_element_type=jnp.float32)
            context = c if context is None else context + c
        c_ref[rows, cols] = context.astype(jnp.bfloat16)


def layer_kernel(n, groups, head_dim, x_ref, wqkv_hbm, wo_hbm, wr_ref, ids_ref, e1_hbm, e3_hbm, e2_hbm, y_ref,
                 wbuf, nbuf, qkv, ubuf, g_own, gbuf, part, acc, w1, w3, w2,
                 b_send, b_recv, c_send, c_recv, c2_send, c2_recv, d_send, d_recv, loc, w_loc, z_send, z_recv, s_send, s_recv, s2_send, s2_recv, w_send, w_recv,
                 u_send, u_recv, a_send, a_recv, g_send, g_recv, *, pieces_u, pieces_a):
    me, group = lax.axis_index('ep'), lax.axis_index('dp')
    pos, core = lax.div(me, 2), lax.rem(me, 2)
    share = wo_hbm.shape[0]
    mats = wbuf.shape[0]
    tok, dim = x_ref.shape
    own, classes = e1_hbm.shape[0], g_own.shape[0]
    hops = classes - 1
    ru = tok // (2 * pieces_u)
    per = pieces_a // pieces_u
    ra = ru // per

    def peer(z):
        return {'ep': lax.rem(z, n) * 2 + core}


    low = math.isqrt(groups) if math.isqrt(groups) ** 2 == groups else groups
    sides = (low, groups // low)
    spots = (lax.rem(group, low), lax.div(group, low))

    def member(f, i, j):
        at = [0, 0]
        at[f] = lax.rem(spots[f] + i + sides[f], sides[f])
        at[1 - f] = lax.rem(spots[1 - f] + j + sides[1 - f], sides[1 - f])
        return at[1] * low + at[0]

    def swap_first(f, piece, sems, i):
        return remote(piece(group), piece(group), sems[0].at[i - 1], sems[1].at[i - 1], {'dp': member(f, i, 0)})

    def swap_then(f, piece, sems, i, j):
        ref, at = piece(member(f, -i, 0)), i * (sides[1 - f] - 1) + j - 1
        return remote(ref, ref, sems[2].at[at], sems[3].at[at], {'dp': member(f, 0, j)})

    def firsts(f):
        return range(1, sides[f])

    def thens(f):
        return range(1, sides[1 - f])

    def swap_start(f, piece, sems):
        for i in firsts(f):
            swap_first(f, piece, sems, i).start()
        for j in thens(f):
            swap_then(f, piece, sems, 0, j).start()

    def swap_relay(f, piece, sems):
        for i in firsts(f):
            swap_first(f, piece, sems, i).wait_recv()
            for j in thens(f):
                swap_then(f, piece, sems, i, j).start()

    def swap_take(f, piece, sems):
        for i in range(sides[f]):
            for j in thens(f):
                swap_then(f, piece, sems, i, j).wait_recv()

    def swap_drain(f, piece, sems):
        for i in firsts(f):
            swap_first(f, piece, sems, i).wait_send()
        for i in range(sides[f]):
            for j in thens(f):
                swap_then(f, piece, sems, i, j).wait_send()

    sibling = {'ep': pos * 2 + (1 - core)}

    def remote(src, dst, send, recv, device):
        return pltpu.make_async_remote_copy(src_ref=src, dst_ref=dst, send_sem=send, recv_sem=recv, device_id=device, device_id_type=MESH)

    barrier = pltpu.get_barrier_semaphore()

    def greet_ring(k, _):
        pl.semaphore_signal(barrier, inc=1, device_id=peer(pos + k), device_id_type=MESH)
        return 0

    def greet_groups(j, _):
        pl.semaphore_signal(barrier, inc=1, device_id={'dp': lax.rem(group + j, groups)}, device_id_type=MESH)
        return 0

    lax.fori_loop(1, n, greet_ring, 0)
    lax.fori_loop(1, groups, greet_groups, 0)
    pl.semaphore_signal(barrier, inc=1, device_id=sibling, device_id_type=MESH)


    parts, whole = max(1, groups // mats), max(1, mats // groups)
    order = sorted(range(n), key=lambda k: min(k, n - k))

    def shard_piece(k, g):
        row = pl.multiple_of(lax.rem(g, parts) * (share // parts), share // parts)
        return wbuf.at[pl.ds(lax.div(g * mats, groups), whole), lax.rem(pos + n - k, n), core, pl.ds(row, share // parts)]

    def along(k):
        return remote(shard_piece(0, group), shard_piece(0, group), b_send.at[k], b_recv.at[k], peer(pos + k))

    def outward(k):
        return k % 2, functools.partial(shard_piece, k), [r.at[k] for r in (c_send, c_recv, c2_send, c2_recv)]

    def across(k):
        block = wbuf.at[:, lax.rem(pos + n - k, n), core]
        return remote(block, block, d_send.at[k], d_recv.at[k], sibling)


    near, away = lax.div(pos, classes) * 2 * own, (1 - lax.div(pos, classes)) * 2 * own
    base = [near + core * own, near + (1 - core) * own, away + core * own, away + (1 - core) * own]
    experts_of = ((e1_hbm, w1), (e3_hbm, w3), (e2_hbm, w2))

    def rows_of(t, d, g):
        size = experts_of[t][0].shape[1] // (2 * groups)
        return pl.ds(pl.multiple_of((g * 2 + d) * size, size), size)

    def load(t):
        return pltpu.make_async_copy(experts_of[t][0], experts_of[t][1].at[pl.ds(base[0], own)], w_loc.at[t])

    def hand(r, t):
        kept = experts_of[t][1].at[pl.ds(base[2 * r], own)]
        return remote(experts_of[t][0] if r == 0 else kept, kept, w_send.at[r, t], w_recv.at[r, t], sibling)

    def fetch(t, d):
        rows = rows_of(t, d, group)
        return remote(experts_of[t][0].at[:, rows], experts_of[t][1].at[pl.ds(base[0], own), rows], z_send.at[t, d], z_recv.at[t, d], peer(pos + n // 2))

    def spread(t, d):
        def expert_piece(g):
            return experts_of[t][1].at[pl.ds(base[2], own), rows_of(t, d, g)]

        return d, expert_piece, [r.at[t, d] for r in (s_send, s_recv, s2_send, s2_recv)]

    def share_out(t, d):
        fetch(t, d).wait_recv()
        swap_start(*spread(t, d))

    def share_on(t, d):
        swap_relay(*spread(t, d))

    def collect(t):
        for d in range(2):
            swap_take(*spread(t, d))
        hand(1, t).start()

    shards = []
    for m, src in enumerate((wqkv_hbm.at[0], wqkv_hbm.at[1], wqkv_hbm.at[2], wo_hbm)):
        shards.append(pltpu.make_async_copy(src, wbuf.at[m, pos, core], loc.at[m]))
        shards[-1].start()
    for t in range(3):
        load(t).start()
    pl.semaphore_wait(barrier, n + groups - 1)
    for m in range(mats):
        shards[m].wait()
    for k in order[1:]:
        along(k).start()
    for t in range(3):
        hand(0, t).start()
    nbuf[...] = rms_norm(x_ref[...]).astype(jnp.bfloat16)
    for s in range(hops + 1):
        part[s] = jnp.zeros(part.shape[1:], jnp.float32)

    across(0).start()
    for i in range(n + 1):
        if i + 1 < n:
            along(order[i + 1]).wait_recv()
            swap_start(*outward(order[i + 1]))
        if i == n // 2 - 1:
            for t in range(3):
                for d in range(2):
                    fetch(t, d).start()
        if i > 1:
            swap_relay(*outward(order[i - 1]))
    share_out(0, 0)
    for k in order[1:]:
        swap_take(*outward(k))
        across(k).start()
    for k in order:
        across(k).wait_recv()
    width = dim // 2

    def project(j, _):
        m, c = lax.div(j, 2), lax.rem(j, 2)
        cols = pl.ds(pl.multiple_of(c * width, width), width)
        qkv[m, :, cols] = jnp.dot(nbuf[...], wbuf[m, :, :, :, cols].reshape(dim, width), preferred_element_type=jnp.float32).astype(jnp.bfloat16)
        return 0

    lax.fori_loop(0, 6, project, 0)
    share_out(0, 1)
    share_on(0, 0)
    pairs = dim // 128

    def heads(i, _):
        attend_pair(qkv.at[0], qkv.at[1], qkv.at[2], nbuf, i, head_dim ** -0.5)

        @pl.when(i == pairs // 4)
        def _():
            share_on(0, 1)

        @pl.when(i == 5 * pairs // 8)
        def _():
            share_out(1, 0)
        return 0

    lax.fori_loop(0, pairs, heads, 0)
    share_on(1, 0)
    for j in range(2):
        cols = slice(j * width, (j + 1) * width)
        mixed = jnp.dot(nbuf[...], wbuf[3, :, :, :, cols].reshape(dim, width), preferred_element_type=jnp.float32)
        y_ref[:, cols] = (x_ref[:, cols].astype(jnp.float32) + mixed).astype(jnp.bfloat16)
    share_out(1, 1)
    z = rms_norm(y_ref[...])
    ubuf[0] = z.astype(jnp.bfloat16)
    logits = lax.dot_general(wr_ref[...], z, (((1,), (1,)), ((), ())), precision=lax.Precision.HIGHEST, preferred_element_type=jnp.float32)
    expert = lax.broadcasted_iota(jnp.int32, logits.shape, 0)
    match = expert == ids_ref[0:1, :]
    for j in range(1, ids_ref.shape[0]):
        match = match | (expert == ids_ref[j:j + 1, :])
    logits = jnp.where(match, logits, -jnp.inf)
    e = jnp.where(match, jnp.exp(logits - jnp.max(logits, axis=0, keepdims=True)), 0.0)
    gates = e / jnp.sum(e, axis=0, keepdims=True)
    layer = gates.shape[0] // n
    for c in range(classes):
        g_own[c] = jnp.concatenate([gates[(c + r * classes) * layer:(c + r * classes + 1) * layer] for r in range(n // classes)], axis=0)


    def u_copy(d, s, p):
        rows = pl.ds((2 * p + d) * ru, ru)
        return remote(ubuf.at[s, rows], ubuf.at[s + 1, rows], u_send.at[d, s, p], u_recv.at[d, s, p], peer(pos + (1 if d == 0 else n - 1)))

    def a_rows(d, p):
        return pl.ds((2 * (p // per) + d) * ru + (p % per) * ra, ra)

    def a_copy(d, s, p):
        rows = a_rows(d, p)
        return remote(part.at[s, rows], acc.at[s - 1, rows], a_send.at[d, s - 1, p], a_recv.at[d, s - 1, p], peer(pos + (n - 1 if d == 0 else 1)))

    def g_copy(d, s):
        target = pos + (s if d == 0 else n - s)
        return remote(g_own.at[lax.rem(target, classes)], gbuf.at[d, s - 1], g_send.at[d, s - 1], g_recv.at[d, s - 1], peer(target))

    for p in range(pieces_u):
        for d in range(2):
            u_copy(d, 0, p).start()

    def experts(s, gates, first, count, start=0, rows=tok):
        here = slice(start, start + rows)
        gates = gates.T[here]

        def one(e, _):
            turn = lax.div(e, own)
            slot = jnp.where(turn == 0, base[0], jnp.where(turn == 1, base[1], jnp.where(turn == 2, base[2], base[3]))) + lax.rem(e, own)
            lane = lax.broadcasted_iota(jnp.int32, gates.shape, 1)
            g = jnp.sum(jnp.where(lane == slot, gates, 0.0), axis=1, keepdims=True)
            u = ubuf[s, here]
            f1 = jnp.dot(u, w1[slot], preferred_element_type=jnp.float32)
            f3 = jnp.dot(u, w3[slot], preferred_element_type=jnp.float32)
            a = (f1 * jax.nn.sigmoid(f1) * f3).astype(jnp.bfloat16)
            for j in range(0, dim, 512):
                o = jnp.dot(a, w2[slot, :, j:j + 512], preferred_element_type=jnp.float32).astype(jnp.bfloat16).astype(jnp.float32)
                part[s, here, j:j + 512] += jnp.where(g != 0.0, g * o, 0.0)
            return 0

        lax.fori_loop(first, first + count, one, 0)

    def gates_of(s):
        if s == 0:
            return g_own[lax.rem(pos, classes)]
        lane = lax.broadcasted_iota(jnp.int32, gbuf.shape[2:], 1)
        return jnp.where(lax.rem(lax.div(lane, ru), 2) == 0, gbuf[0, s - 1], gbuf[1, s - 1])

    def forward(s, first=0, last=pieces_u):
        for p in range(first, last):
            for d in range(2):
                u_copy(d, s - 1, p).wait_recv()
                if s < hops:
                    u_copy(d, s, p).start()

    for t in range(3):
        load(t).wait()
    for s in range(1, hops + 1):
        for d in range(2):
            g_copy(d, s).start()
    share_on(1, 1)
    share_out(2, 0)
    experts(0, gates_of(0), 0, own)
    for t in range(3):
        hand(0, t).wait()
    collect(0)
    experts(0, gates_of(0), own, own)
    share_on(2, 0)
    share_out(2, 1)
    forward(1)
    for s in range(1, hops + 1):
        for d in range(2):
            g_copy(d, s).wait()
    experts(1, gates_of(1), 0, own)
    share_on(2, 1)
    collect(1)
    experts(1, gates_of(1), own, own)
    forward(2)
    experts(2, gates_of(2), 0, 2 * own)
    collect(2)
    for s in range(3, hops):
        forward(s)
    for p in range(pieces_u):
        forward(hops, p, p + 1)
        experts(hops, gates_of(hops), 0, 2 * own, p * 2 * ru, 2 * ru)
    for t in range(3):
        hand(1, t).wait_recv()
    for p in range(pieces_u):
        experts(hops, gates_of(hops), 2 * own, 2 * own, p * 2 * ru, 2 * ru)
        for q in range(p * per, (p + 1) * per):
            for d in range(2):
                a_copy(d, hops, q).start()

    for s in range(hops - 1, -1, -1):
        experts(s, gates_of(s), 2 * own, 2 * own)
        for p in range(pieces_a):
            for d in range(2):
                rows = a_rows(d, p)
                a_copy(d, s + 1, p).wait_recv()
                if s > 0:
                    part[s, rows] += acc[s, rows]
                    a_copy(d, s, p).start()
                else:
                    y_ref[rows] = (y_ref[rows].astype(jnp.float32) + (part[s, rows] + acc[s, rows])).astype(y_ref.dtype)


    for k in order:
        across(k).wait_send()
        if k:
            along(k).wait_send()
            swap_drain(*outward(k))

    for t in range(3):
        for d in range(2):
            swap_drain(*spread(t, d))
    for t in range(3):
        hand(1, t).wait_send()
        for d in range(2):
            fetch(t, d).wait_send()
    for s in range(hops):
        for d in range(2):
            for p in range(pieces_u):
                u_copy(d, s, p).wait_send()
            for p in range(pieces_a):
                a_copy(d, s + 1, p).wait_send()


def layer(x, w_qkv, w_out, w_router_t, ids_t, w_one, w_three, w_two, n, groups, head_dim):
    tok, dim = x.shape
    own, _, ff = w_one.shape
    classes = n // 2
    hops, total = classes - 1, 4 * own
    pieces_u, pieces_a = 2, 4
    dma = pltpu.SemaphoreType.DMA
    any_spec = pl.BlockSpec(memory_space=pl.ANY)
    vmem = pl.BlockSpec(memory_space=pltpu.VMEM)
    bf16, f32 = jnp.bfloat16, jnp.float32
    return pl.pallas_call(
        functools.partial(layer_kernel, n, groups, head_dim, pieces_u=pieces_u, pieces_a=pieces_a),
        out_shape=jax.ShapeDtypeStruct((tok, dim), bf16),
        in_specs=[vmem, any_spec, any_spec, vmem, vmem, any_spec, any_spec, any_spec],
        out_specs=vmem,
        scratch_shapes=[
            pltpu.VMEM((4, n, 2, w_out.shape[0], dim), bf16),
            pltpu.VMEM((tok, dim), bf16),
            pltpu.VMEM((3, tok, dim), bf16),
            pltpu.VMEM((hops + 1, tok, dim), bf16),
            pltpu.VMEM((classes, total, tok), f32),
            pltpu.VMEM((2, hops, total, tok), f32),
            pltpu.VMEM((hops + 1, tok, dim), f32),
            pltpu.VMEM((hops, tok, dim), f32),
            pltpu.VMEM((total, dim, ff), bf16),
            pltpu.VMEM((total, dim, ff), bf16),
            pltpu.VMEM((total, ff, dim), bf16),
            dma((n,)), dma((n,)), *(dma((n, groups)) for _ in range(4)), dma((n,)), dma((n,)), dma((4,)), dma((3,)),
            dma((3, 2)), dma((3, 2)), *(dma((3, 2, groups)) for _ in range(4)), dma((2, 3)), dma((2, 3)),
            dma((2, hops, pieces_u)), dma((2, hops, pieces_u)),
            dma((2, hops, pieces_a)), dma((2, hops, pieces_a)),
            dma((2, hops)), dma((2, hops)),
        ],
        compiler_params=pltpu.CompilerParams(collective_id=1, has_side_effects=True, vmem_limit_bytes=67_000_000),
        name='layer_ring',
    )(x, w_qkv, w_out, w_router_t, ids_t, w_one, w_three, w_two)


def solution(mesh):
    tok_spec = P(('dp', 'ep'))
    row_spec = P('ep')
    n = mesh.shape['ep'] // 2
    groups = mesh.shape['dp']

    def local_layer(tokens, w_query, w_key, w_value, w_out, w_router, w_one, w_three, w_two, expert_ids):
        tok, dim = tokens.shape[0] * tokens.shape[1], tokens.shape[2]
        flat = jnp.stack([w_query, w_key, w_value]).reshape(3, w_query.shape[0], -1)
        ids_t = expert_ids.reshape(tok, -1).T
        out = layer(tokens.reshape(tok, dim), flat, w_out, w_router.T, ids_t, w_one, w_three, w_two, n, groups, w_query.shape[2])
        return out.reshape(tokens.shape)

    return jax.shard_map(local_layer, mesh=mesh, in_specs=(tok_spec, row_spec, row_spec, row_spec, row_spec, P(), row_spec, row_spec, row_spec, tok_spec), out_specs=tok_spec, check_vma=False)
```
